8 devices in a mesh: dp: 2 (over z, y), fsdp: 4 (over x, core).
Axes of the slice: x: 2, y: 2, z: 1, core: 2. Of those that a mesh axis runs over, the one named last changes fastest.
Arguments:
- g_layer: float32 [8, 6, 256, 896], P(('dp', 'fsdp'))
- g_down: float32 [8, 256, 4864], P(('dp', 'fsdp'))
- g_norm: float32 [8, 4, 896], P(('dp', 'fsdp'))
- g_embed: float32 [8, 256, 896], P(('dp', 'fsdp'))
- layer_w: float32 [6, 256, 896], P(None, 'fsdp')
- layer_m: float32 [6, 256, 896], P(None, 'fsdp')
- layer_v: float32 [6, 256, 896], P(None, 'fsdp')
- down_w: float32 [256, 4864], P('fsdp')
- down_m: float32 [256, 4864], P('fsdp')
- down_v: float32 [256, 4864], P('fsdp')
- norm_w: float32 [4, 896], P(None, 'fsdp')
- norm_m: float32 [4, 896], P(None, 'fsdp')
- norm_v: float32 [4, 896], P(None, 'fsdp')
- embed_w: float32 [256, 896], P('fsdp')
- embed_m: float32 [256, 896], P('fsdp')
- embed_v: float32 [256, 896], P('fsdp')
Outputs:
- output 1: float32 [6, 256, 896], P(None, 'fsdp')
- output 2: float32 [6, 256, 896], P(None, 'fsdp')
- output 3: float32 [6, 256, 896], P(None, 'fsdp')
- output 4: bfloat16 [6, 256, 896], P(None, 'fsdp')
- output 5: float32 [256, 4864], P('fsdp')
- output 6: float32 [256, 4864], P('fsdp')
- output 7: float32 [256, 4864], P('fsdp')
- output 8: bfloat16 [256, 4864], P('fsdp')
- output 9: float32 [4, 896], P(None, 'fsdp')
- output 10: float32 [4, 896], P(None, 'fsdp')
- output 11: float32 [4, 896], P(None, 'fsdp')
- output 12: bfloat16 [4, 896], P(None, 'fsdp')
- output 13: float32 [256, 896], P('fsdp')
- output 14: float32 [256, 896], P('fsdp')
- output 15: float32 [256, 896], P('fsdp')
- output 16: bfloat16 [256, 896], P('fsdp')
All inputs are finite; a program needn't handle non-finite values.
Results may differ from the reference program's by a relative error of at most 0.001.
Values sent between devices are 32-bit elements.
A program may use at most 1 GiB of HBM per device.

```python
import math
import jax
import jax.numpy as jnp

D = 896
FF = 4864
LAYER_ROWS = 256
EMB_ROWS = 256
DEVICES = 8
OPT_STEP = 20

ADAM_BETA1 = 0.9
ADAM_BETA2 = 0.95
ADAM_EPS = 1e-8
LEARN_RATE = 4e-4
WEIGHT_DECAY = 0.1
CLIP_EPS = 1e-6
BIAS_ONE = 1.0 - ADAM_BETA1 ** OPT_STEP
BIAS_TWO = 1.0 - ADAM_BETA2 ** OPT_STEP
NORM_TARGET = 4.0


def draw_group(key_list, arr_shape, grad_share, init_std, init_mean):
    elem_count = math.prod(arr_shape)
    grad_scale = (grad_share * NORM_TARGET ** 2 * DEVICES / elem_count) ** 0.5
    unit_scale = (grad_share / elem_count) ** 0.5
    grad_all = grad_scale * jax.random.normal(key_list[0], (DEVICES,) + arr_shape, jnp.float32)
    master = init_mean + init_std * jax.random.normal(key_list[1], arr_shape, jnp.float32)
    exp_avg = 0.06 * unit_scale * jax.random.normal(key_list[2], arr_shape, jnp.float32)
    exp_avg_sq = 0.05 * unit_scale * unit_scale * jax.random.uniform(key_list[3], arr_shape, jnp.float32, 0.5, 1.5)
    return grad_all, master, exp_avg, exp_avg_sq


def setup_inputs(seed: int = 0) -> dict:
    key_list = jax.random.split(jax.random.key(seed), 16)
    layer_draw = draw_group(key_list[0:4], (6, LAYER_ROWS, D), 0.45, 0.02, 0.0)
    down_draw = draw_group(key_list[4:8], (LAYER_ROWS, FF), 0.2, 0.02, 0.0)
    norm_draw = draw_group(key_list[8:12], (4, D), 0.05, 0.1, 1.0)
    embed_draw = draw_group(key_list[12:16], (EMB_ROWS, D), 0.3, 0.02, 0.0)
    return {
        "g_layer": layer_draw[0], "g_down": down_draw[0], "g_norm": norm_draw[0], "g_embed": embed_draw[0],
        "layer_w": layer_draw[1], "layer_m": layer_draw[2], "layer_v": layer_draw[3],
        "down_w": down_draw[1], "down_m": down_draw[2], "down_v": down_draw[3],
        "norm_w": norm_draw[1], "norm_m": norm_draw[2], "norm_v": norm_draw[3],
        "embed_w": embed_draw[1], "embed_m": embed_draw[2], "embed_v": embed_draw[3],
    }


def adamw_step(grad_mean, master, exp_avg, exp_avg_sq, clip_coef, decay_rate):
    clipped = clip_coef * grad_mean
    avg_new = ADAM_BETA1 * exp_avg + (1.0 - ADAM_BETA1) * clipped
    sq_new = ADAM_BETA2 * exp_avg_sq + (1.0 - ADAM_BETA2) * clipped * clipped
    step_dir = (avg_new / BIAS_ONE) / (jnp.sqrt(sq_new / BIAS_TWO) + ADAM_EPS)
    master_new = master - LEARN_RATE * (step_dir + decay_rate * master)
    return master_new, avg_new, sq_new, master_new.astype(jnp.bfloat16)


def reference(g_layer, g_down, g_norm, g_embed, layer_w, layer_m, layer_v, down_w, down_m, down_v, norm_w, norm_m, norm_v, embed_w, embed_m, embed_v):
    layer_mean = jnp.sum(g_layer, axis=0) / DEVICES
    down_mean = jnp.sum(g_down, axis=0) / DEVICES
    norm_mean = jnp.sum(g_norm, axis=0) / DEVICES
    embed_mean = jnp.sum(g_embed, axis=0) / DEVICES
    sq_total = (jnp.sum(layer_mean * layer_mean) + jnp.sum(down_mean * down_mean)
                + jnp.sum(norm_mean * norm_mean) + jnp.sum(embed_mean * embed_mean))
    global_norm = jnp.sqrt(sq_total)
    clip_coef = jnp.minimum(1.0, 1.0 / (global_norm + CLIP_EPS))
    layer_new = adamw_step(layer_mean, layer_w, layer_m, layer_v, clip_coef, WEIGHT_DECAY)
    down_new = adamw_step(down_mean, down_w, down_m, down_v, clip_coef, WEIGHT_DECAY)
    norm_new = adamw_step(norm_mean, norm_w, norm_m, norm_v, clip_coef, WEIGHT_DECAY)
    embed_new = adamw_step(embed_mean, embed_w, embed_m, embed_v, clip_coef, 0.0)
    return (layer_new[0], layer_new[1], layer_new[2], layer_new[3],
            down_new[0], down_new[1], down_new[2], down_new[3],
            norm_new[0], norm_new[1], norm_new[2], norm_new[3],
            embed_new[0], embed_new[1], embed_new[2], embed_new[3])
```

```python
import jax
import jax.numpy as jnp
from jax import lax
from jax.experimental import pallas as pl
from jax.experimental.pallas import tpu as pltpu
from jax.sharding import PartitionSpec as P

ADAM_BETA1 = 0.9
ADAM_BETA2 = 0.95
ADAM_EPS = 1e-8
LEARN_RATE = 4e-4
WEIGHT_DECAY = 0.1
CLIP_EPS = 1e-6
OPT_STEP = 20
BIAS_ONE = 1.0 - ADAM_BETA1 ** OPT_STEP
BIAS_TWO = 1.0 - ADAM_BETA2 ** OPT_STEP

MESH = pl.DeviceIdType.MESH
LAYER, DOWN, NORM, EMBED = range(4)
DECAYS = (WEIGHT_DECAY, WEIGHT_DECAY, WEIGHT_DECAY, 0.0)
SHARES = ((6, 64, 896), (64, 4864), (4, 224), (64, 896))
WINDOWS = ((6, 64, 896), (64, 4864), (4, 384), (64, 896))
FIRST = slice(0, 8)

GROUPS = ((EMBED, FIRST), (EMBED, slice(8, 64)), (NORM, None), (DOWN, slice(0, 64)), (LAYER, None))


def plan():
    chunks = [(EMBED, (slice(r, r + 8),), int(r > 0)) for r in range(0, 64, 8)]
    chunks.append((NORM, (), 2))
    cuts = (0, 1024, 2048, 3072, 3968, 4864)
    chunks += [(DOWN, (slice(r, r + 8), slice(a, b)), 3) for r in range(0, 64, 8) for a, b in zip(cuts, cuts[1:])]
    chunks += [(LAYER, (l, slice(r, r + 8)), 4) for l in range(6) for r in range(0, 64, 8)]
    return chunks


CHUNKS = plan()
X_AHEAD, Y_BEHIND = 8, 5
X_RING, Y_RING = 2 * X_AHEAD + 2, 2 * Y_BEHIND + 2


def at(ref, index):
    return ref.at[tuple(pl.ds(i.start, i.stop - i.start) if isinstance(i, slice) else i for i in index)] if index else ref


def tile_sum(value):
    rows, columns = value.shape
    parts = [value[r:r + 8, c:c + 128] for r in range(0, rows, 8) for c in range(0, columns, 128)]
    while len(parts) > 1:
        parts = [a + b for a, b in zip(parts[::2], parts[1::2])] + parts[len(parts) // 2 * 2:]
    return parts[0]


def reduce_kernel(*refs):
    grads, states = refs[:4], refs[4:16]
    means, copies, clip = refs[16:20], refs[20:32], refs[32]
    far, near, x_in, y_in = (refs[33 + 4 * i:37 + 4 * i] for i in range(4))
    (first, norms, acc, first_sem, group_sem, state_sem, pair_send, x_send, y_send, x_recv, y_recv,
     norm_send, norm_recv) = refs[49:]

    dp, me = lax.axis_index("dp"), lax.axis_index("fsdp")
    partner = me + 1 - 2 * lax.rem(me, 2)
    across = lax.rem(me + 2, 4)
    diagonal = lax.rem(partner + 2, 4)
    other = 1 - dp
    peers = ((dp, across), (dp, diagonal), (dp, partner))
    held = (far, near)

    def share(array, fsdp, rows=None):
        ref = grads[array].at[0]
        if array == NORM:
            start = jnp.minimum((fsdp * 7) // 4, 4)
            return ref.at[:, pl.ds(pl.multiple_of(start * 128, 128), 384)]
        rows = rows or slice(0, 64)
        window = pl.ds(pl.multiple_of(fsdp * 64 + rows.start, 8), rows.stop - rows.start)
        return ref.at[:, window, :] if array == LAYER else ref.at[window, :]

    def slot(which, g, i):
        array, rows = GROUPS[g]
        ref = held[which][array].at[i]
        return ref if rows is None else ref.at[pl.ds(rows.start, rows.stop - rows.start), :]

    def load(which, g):
        array, rows = GROUPS[g]
        return pltpu.make_async_copy(
            share(array, (across, me)[which], rows), slot(which, g, 0), group_sem.at[which, g])

    def load_first(which):
        return pltpu.make_async_copy(
            share(EMBED, (diagonal, partner)[which], FIRST), first.at[which], first_sem)

    def pair(which, g):
        array, rows = GROUPS[g]
        return pltpu.make_async_remote_copy(
            src_ref=share(array, (diagonal, partner)[which], rows) if g else first.at[which],
            dst_ref=slot(which, g, 1), send_sem=pair_send, recv_sem=group_sem.at[which, g],
            device_id=(dp, partner), device_id_type=MESH)

    def over_x(c):
        array, index, _ = CHUNKS[c]
        return pltpu.make_async_remote_copy(
            src_ref=at(far[array].at[0], index), dst_ref=at(x_in[array], index),
            send_sem=x_send, recv_sem=x_recv.at[c % X_RING], device_id=(dp, across), device_id_type=MESH)

    def over_y(c):
        array, index, _ = CHUNKS[c]
        return pltpu.make_async_remote_copy(
            src_ref=at(near[array].at[0], index), dst_ref=at(y_in[array], index),
            send_sem=y_send, recv_sem=y_recv.at[c % Y_RING], device_id=(other, me), device_id_type=MESH)

    def norm_to(i):
        return pltpu.make_async_remote_copy(
            src_ref=norms.at[me], dst_ref=norms.at[me], send_sem=norm_send, recv_sem=norm_recv.at[i],
            device_id=peers[i], device_id_type=MESH)

    barrier = pltpu.get_barrier_semaphore()
    for device in ((other, me),) + peers:
        pl.semaphore_signal(barrier, inc=1, device_id=device, device_id_type=MESH)
    for which in (0, 1):
        load_first(which).start()
    for g in range(len(GROUPS)):
        for which in (0, 1):
            load(which, g).start()
    acc[...] = jnp.zeros_like(acc)
    pltpu.make_async_copy(first, first, first_sem).wait()
    pl.semaphore_wait(barrier, 4)
    for g in range(len(GROUPS)):
        for which in (0, 1):
            pair(which, g).start()
    for s, d in zip(states, copies):
        pltpu.make_async_copy(s, d, state_sem).start()

    ready = set()

    def need(which, g):
        if (which, g) not in ready:
            ready.add((which, g))
            array, rows = GROUPS[g]
            ref = held[which][array]
            if rows is not None:
                ref = ref.at[:, pl.ds(rows.start, rows.stop - rows.start), :]
            pltpu.make_async_copy(ref, ref, group_sem.at[which, g]).wait()

    def send_x(c):
        array, index, g = CHUNKS[c]
        need(0, g)
        ref = at(far[array].at[0], index)
        ref[...] = ref[...] + at(far[array].at[1], index)[...]
        over_x(c).start()

    def send_y(c):
        array, index, g = CHUNKS[c]
        need(1, g)
        over_x(c).wait_recv()
        ref = at(near[array].at[0], index)
        ref[...] = (ref[...] + at(near[array].at[1], index)[...]) + at(x_in[array], index)[...]
        over_y(c).start()

    def finish(c):
        array, index, _ = CHUNKS[c]
        over_y(c).wait_recv()
        mean = (at(near[array].at[0], index)[...] + at(y_in[array], index)[...]) * (1.0 / 8.0)
        if array == NORM:
            for f, skip in enumerate((0, 96, 64, 160)):
                @pl.when(me == f)
                def _():
                    mine = pltpu.roll(mean, (384 - skip) % 384, axis=1)
                    mine = jnp.where(lax.broadcasted_iota(jnp.int32, (4, 384), 1) < 224, mine, 0.0)
                    means[NORM][...] = mine[:, :224]
                    square = mine * mine
                    acc[0:4, :] = acc[0:4, :] + (square[:, :128] + square[:, 128:256])
        else:
            at(means[array], index)[...] = mean
            total = acc[...] + tile_sum(mean * mean)
            if c < len(CHUNKS) - 1:
                acc[...] = total
            else:
                norms[me] = total

    count = len(CHUNKS)
    for step in range(count + X_AHEAD + Y_BEHIND):
        if step < count:
            send_x(step)
        if 0 <= step - X_AHEAD < count:
            send_y(step - X_AHEAD)
        if 0 <= step - X_AHEAD - Y_BEHIND < count:
            finish(step - X_AHEAD - Y_BEHIND)
    for i in range(3):
        norm_to(i).start()

    for s, d in zip(states, copies):
        pltpu.make_async_copy(s, d, state_sem).wait()
    for array in range(4):
        for which in (0, 1):
            ref = held[which][array].at[0]
            pltpu.make_async_remote_copy(
                src_ref=ref, dst_ref=ref, send_sem=pair_send, recv_sem=norm_recv.at[0],
                device_id=(dp, partner), device_id_type=MESH).wait_send()
        pltpu.make_async_remote_copy(
            src_ref=far[array].at[0], dst_ref=x_in[array], send_sem=x_send, recv_sem=x_recv.at[0],
            device_id=(dp, across), device_id_type=MESH).wait_send()
        pltpu.make_async_remote_copy(
            src_ref=near[array].at[0], dst_ref=y_in[array], send_sem=y_send, recv_sem=y_recv.at[0],
            device_id=(other, me), device_id_type=MESH).wait_send()
    for i in range(3):
        norm_to(i).wait_send()
    for i in range(3):
        norm_to(i).wait_recv()
    total = (norms[0] + norms[1]) + (norms[2] + norms[3])
    total = jnp.sum(jnp.sum(total, axis=0, keepdims=True), axis=1, keepdims=True)
    norm = jnp.sqrt(jnp.broadcast_to(total, (8, 128)))
    clip[...] = jnp.minimum(1.0, 1.0 / (norm + CLIP_EPS))


def adamw(mean, master, exp_avg, exp_avg_sq, clip, decay):
    clipped = clip * mean
    avg_new = ADAM_BETA1 * exp_avg + (1.0 - ADAM_BETA1) * clipped
    sq_new = ADAM_BETA2 * exp_avg_sq + (1.0 - ADAM_BETA2) * clipped * clipped
    step_dir = (avg_new / BIAS_ONE) / (jnp.sqrt(sq_new / BIAS_TWO) + ADAM_EPS)
    master_new = master - LEARN_RATE * (step_dir + decay * master)
    return master_new, avg_new, sq_new, master_new.astype(jnp.bfloat16)


def update_kernel(*refs):
    means, states, clip_ref = refs[:4], refs[4:16], refs[16]
    outs, bufs, sem = refs[17:33], refs[33:49], refs[49]
    clip = clip_ref[...]

    def rows(array, index):
        ins = [means[array]] + list(states[3 * array:3 * array + 3])
        ins = [r[index] for r in ins]
        height, width = ins[0].shape
        scale = jnp.concatenate([clip[:height]] * -(-width // 128), axis=1)[:, :width]
        for o, value in zip(bufs[4 * array:4 * array + 4], adamw(*ins, scale, DECAYS[array])):
            o[index] = value

    def send(array, index):
        for k in range(4 * array, 4 * array + 4):
            pltpu.make_async_copy(at(bufs[k], index), at(outs[k], index), sem.at[k % SEMS]).start()

    for l in range(6):
        for r in range(0, 64, 8):
            rows(LAYER, (l, slice(r, r + 8)))
        send(LAYER, (l,))
    for r in range(0, 64, 8):
        rows(DOWN, (slice(r, r + 8),))
        send(DOWN, (slice(r, r + 8),))
    for r in range(0, 64, 8):
        rows(EMBED, (slice(r, r + 8),))
    send(EMBED, ())
    rows(NORM, (slice(0, 4),))
    send(NORM, ())
    for k in range(16):
        pltpu.make_async_copy(bufs[k], outs[k], sem.at[k % SEMS]).wait()


SEMS = 1


def solution(mesh):
    grad_four = P(("dp", "fsdp"), None, None, None)
    grad_three = P(("dp", "fsdp"), None, None)
    layer_spec = P(None, "fsdp", None)
    down_spec = P("fsdp", None)
    norm_spec = P(None, "fsdp")
    embed_spec = P("fsdp", None)
    any_spec = pl.BlockSpec(memory_space=pl.ANY)
    vmem_spec = pl.BlockSpec(memory_space=pltpu.VMEM)
    dma = pltpu.SemaphoreType.DMA
    f32 = jnp.float32

    def local_update(*args):
        state_shapes = [s for s in SHARES for _ in range(3)]
        results = pl.pallas_call(
            reduce_kernel,
            out_shape=tuple(pltpu.VMEM(s, f32) for s in list(SHARES) + state_shapes + [(8, 128)]),
            in_specs=[any_spec] * 16,
            out_specs=(vmem_spec,) * 17,
            scratch_shapes=[pltpu.VMEM(lead + s, f32) for lead in ((2,), (2,), (), ()) for s in WINDOWS] + [
                pltpu.VMEM((2, 8, 896), f32), pltpu.VMEM((4, 8, 128), f32), pltpu.VMEM((8, 128), f32),
                dma, dma((2, len(GROUPS))), dma, dma, dma, dma, dma((X_RING,)), dma((Y_RING,)), dma, dma((3,)),
            ],
            compiler_params=pltpu.CompilerParams(
                collective_id=0, has_side_effects=True, vmem_limit_bytes=24 * 1024 * 1024),
            name="reduce_grads",
        )(*(pltpu.with_memory_space_constraint(a, pltpu.HBM) for a in args))
        out_shapes = [(s, d) for s in SHARES for d in (f32, f32, f32, jnp.bfloat16)]
        return pl.pallas_call(
            update_kernel,
            out_shape=tuple(jax.ShapeDtypeStruct(s, d) for s, d in out_shapes),
            in_specs=[vmem_spec] * 17,
            out_specs=(any_spec,) * 16,
            scratch_shapes=[pltpu.VMEM(s, d) for s, d in out_shapes] + [dma((SEMS,))],
            compiler_params=pltpu.CompilerParams(vmem_limit_bytes=16 * 1024 * 1024),
            name="adamw_update",
        )(*(pltpu.with_memory_space_constraint(r, pltpu.VMEM) for r in results))

    in_specs = (grad_four, grad_three, grad_three, grad_three,
                layer_spec, layer_spec, layer_spec, down_spec, down_spec, down_spec,
                norm_spec, norm_spec, norm_spec, embed_spec, embed_spec, embed_spec)
    out_specs = (layer_spec,) * 4 + (down_spec,) * 4 + (norm_spec,) * 4 + (embed_spec,) * 4
    return jax.shard_map(local_update, mesh=mesh, in_specs=in_specs, out_specs=out_specs, check_vma=False)
```

```python
import jax
import jax.numpy as jnp
from jax import lax
from jax.experimental import pallas as pl
from jax.experimental.pallas import tpu as pltpu
from jax.sharding import PartitionSpec as P

ADAM_BETA1 = 0.9
ADAM_BETA2 = 0.95
ADAM_EPS = 1e-8
LEARN_RATE = 4e-4
WEIGHT_DECAY = 0.1
CLIP_EPS = 1e-6
OPT_STEP = 20
BIAS_ONE = 1.0 - ADAM_BETA1 ** OPT_STEP
BIAS_TWO = 1.0 - ADAM_BETA2 ** OPT_STEP

MESH = pl.DeviceIdType.MESH
LAYER, DOWN, NORM, EMBED = range(4)
DECAYS = (WEIGHT_DECAY, WEIGHT_DECAY, WEIGHT_DECAY, 0.0)
SHARES = ((6, 64, 896), (64, 4864), (4, 224), (64, 896))
WINDOWS = ((6, 64, 896), (64, 4864), (4, 384), (64, 896))
FIRST = slice(0, 8)

GROUPS = ([(EMBED, None, FIRST), (EMBED, None, slice(8, 64)), (NORM, None, None)]
          + [(DOWN, None, slice(r, r + 8)) for r in range(0, 64, 8)] + [(LAYER, l, None) for l in range(6)])
PAIR_AHEAD = 2
PAIR_RING = 2 * PAIR_AHEAD


def plan():
    chunks = [(EMBED, (slice(r, r + 8),), int(r > 0)) for r in range(0, 64, 8)]
    chunks.append((NORM, (), 2))
    cuts = (0, 1024, 2048, 3072, 3968, 4864)
    chunks += [(DOWN, (slice(r, r + 8), slice(a, b)), 3 + r // 8) for r in range(0, 64, 8) for a, b in zip(cuts, cuts[1:])]
    chunks += [(LAYER, (l, slice(r, r + 8)), 11 + l) for l in range(6) for r in range(0, 64, 8)]
    return chunks


CHUNKS = plan()
X_AHEAD, Y_BEHIND = 8, 5
X_RING, Y_RING = 2 * X_AHEAD + 2, 2 * Y_BEHIND + 2


def at(ref, index):
    return ref.at[tuple(pl.ds(i.start, i.stop - i.start) if isinstance(i, slice) else i for i in index)] if index else ref


def tile_sum(value):
    rows, columns = value.shape
    parts = [value[r:r + 8, c:c + 128] for r in range(0, rows, 8) for c in range(0, columns, 128)]
    while len(parts) > 1:
        parts = [a + b for a, b in zip(parts[::2], parts[1::2])] + parts[len(parts) // 2 * 2:]
    return parts[0]


def reduce_kernel(*refs):
    grads, states = refs[:4], refs[4:16]
    means, copies, clip = refs[16:20], refs[20:32], refs[32]
    far, near, x_in, y_in = (refs[33 + 4 * i:37 + 4 * i] for i in range(4))
    (first, norms, acc, first_sem, group_sem, state_sem, pair_send, x_send, y_send, x_recv, y_recv,
     norm_send, norm_recv) = refs[49:]

    dp, me = lax.axis_index("dp"), lax.axis_index("fsdp")
    partner = me + 1 - 2 * lax.rem(me, 2)
    across = lax.rem(me + 2, 4)
    diagonal = lax.rem(partner + 2, 4)
    other = 1 - dp
    peers = ((dp, across), (dp, diagonal), (dp, partner))
    held = (far, near)

    def share(array, fsdp, layer=None, rows=None):
        ref = grads[array].at[0]
        if array == NORM:
            start = jnp.minimum((fsdp * 7) // 4, 4)
            return ref.at[:, pl.ds(pl.multiple_of(start * 128, 128), 384)]
        rows = rows or slice(0, 64)
        window = pl.ds(pl.multiple_of(fsdp * 64 + rows.start, 8), rows.stop - rows.start)
        return ref.at[layer, window, :] if array == LAYER else ref.at[window, :]

    def slot(which, g, i):
        array, layer, rows = GROUPS[g]
        ref = held[which][array]
        lead = i if i is not None else slice(0, 2)
        return at(ref, (lead, layer) if array == LAYER else (lead, rows) if rows is not None else (lead,))

    def load(which, g):
        array, layer, rows = GROUPS[g]
        return pltpu.make_async_copy(
            share(array, (across, me)[which], layer, rows), slot(which, g, 0), group_sem.at[which, g % PAIR_RING])

    def load_first(which):
        return pltpu.make_async_copy(
            share(EMBED, (diagonal, partner)[which], None, FIRST), first.at[which], first_sem)

    def pair(which, g):
        array, layer, rows = GROUPS[g]
        return pltpu.make_async_remote_copy(
            src_ref=share(array, (diagonal, partner)[which], layer, rows) if g else first.at[which],
            dst_ref=slot(which, g, 1), send_sem=pair_send, recv_sem=group_sem.at[which, g % PAIR_RING],
            device_id=(dp, partner), device_id_type=MESH)

    def over_x(c):
        array, index, _ = CHUNKS[c]
        return pltpu.make_async_remote_copy(
            src_ref=at(far[array].at[0], index), dst_ref=at(x_in[array], index),
            send_sem=x_send, recv_sem=x_recv.at[c % X_RING], device_id=(dp, across), device_id_type=MESH)

    def over_y(c):
        array, index, _ = CHUNKS[c]
        return pltpu.make_async_remote_copy(
            src_ref=at(near[array].at[0], index), dst_ref=at(y_in[array], index),
            send_sem=y_send, recv_sem=y_recv.at[c % Y_RING], device_id=(other, me), device_id_type=MESH)

    def norm_to(i):
        return pltpu.make_async_remote_copy(
            src_ref=norms.at[me], dst_ref=norms.at[me], send_sem=norm_send, recv_sem=norm_recv.at[i],
            device_id=peers[i], device_id_type=MESH)

    barrier = pltpu.get_barrier_semaphore()
    for device in ((other, me),) + peers:
        pl.semaphore_signal(barrier, inc=1, device_id=device, device_id_type=MESH)
    for which in (0, 1):
        load_first(which).start()
    for g in range(PAIR_AHEAD):
        for which in (0, 1):
            load(which, g).start()
    acc[...] = jnp.zeros_like(acc)
    pltpu.make_async_copy(first, first, first_sem).wait()
    pl.semaphore_wait(barrier, 4)
    for g in range(PAIR_AHEAD):
        for which in (0, 1):
            pair(which, g).start()
    for s, d in zip(states, copies):
        pltpu.make_async_copy(s, d, state_sem).start()

    ready = set()

    def need(which, g):
        if (which, g) not in ready:
            ready.add((which, g))
            ref = slot(which, g, None)
            pltpu.make_async_copy(ref, ref, group_sem.at[which, g % PAIR_RING]).wait()
            if g + PAIR_AHEAD < len(GROUPS):
                pair(which, g + PAIR_AHEAD).start()
                load(which, g + PAIR_AHEAD).start()

    def send_x(c):
        array, index, g = CHUNKS[c]
        need(0, g)
        ref = at(far[array].at[0], index)
        ref[...] = ref[...] + at(far[array].at[1], index)[...]
        over_x(c).start()

    def send_y(c):
        array, index, g = CHUNKS[c]
        need(1, g)
        over_x(c).wait_recv()
        ref = at(near[array].at[0], index)
        ref[...] = (ref[...] + at(near[array].at[1], index)[...]) + at(x_in[array], index)[...]
        over_y(c).start()

    def finish(c):
        array, index, _ = CHUNKS[c]
        over_y(c).wait_recv()
        mean = (at(near[array].at[0], index)[...] + at(y_in[array], index)[...]) * (1.0 / 8.0)
        if array == NORM:
            for f, skip in enumerate((0, 96, 64, 160)):
                @pl.when(me == f)
                def _():
                    mine = pltpu.roll(mean, (384 - skip) % 384, axis=1)
                    mine = jnp.where(lax.broadcasted_iota(jnp.int32, (4, 384), 1) < 224, mine, 0.0)
                    means[NORM][...] = mine[:, :224]
                    square = mine * mine
                    acc[0:4, :] = acc[0:4, :] + (square[:, :128] + square[:, 128:256])
        else:
            at(means[array], index)[...] = mean
            total = acc[...] + tile_sum(mean * mean)
            if c < len(CHUNKS) - 1:
                acc[...] = total
            else:
                norms[me] = total

    count = len(CHUNKS)
    for step in range(count + X_AHEAD + Y_BEHIND):
        if step < count:
            send_x(step)
        if 0 <= step - X_AHEAD < count:
            send_y(step - X_AHEAD)
        if 0 <= step - X_AHEAD - Y_BEHIND < count:
            finish(step - X_AHEAD - Y_BEHIND)
    for i in range(3):
        norm_to(i).start()

    for s, d in zip(states, copies):
        pltpu.make_async_copy(s, d, state_sem).wait()
    for array in range(4):
        for which in (0, 1):
            ref = held[which][array].at[0]
            pltpu.make_async_remote_copy(
                src_ref=ref, dst_ref=ref, send_sem=pair_send, recv_sem=norm_recv.at[0],
                device_id=(dp, partner), device_id_type=MESH).wait_send()
        pltpu.make_async_remote_copy(
            src_ref=far[array].at[0], dst_ref=x_in[array], send_sem=x_send, recv_sem=x_recv.at[0],
            device_id=(dp, across), device_id_type=MESH).wait_send()
        pltpu.make_async_remote_copy(
            src_ref=near[array].at[0], dst_ref=y_in[array], send_sem=y_send, recv_sem=y_recv.at[0],
            device_id=(other, me), device_id_type=MESH).wait_send()
    for i in range(3):
        norm_to(i).wait_send()
    for i in range(3):
        norm_to(i).wait_recv()
    total = (norms[0] + norms[1]) + (norms[2] + norms[3])
    total = jnp.sum(jnp.sum(total, axis=0, keepdims=True), axis=1, keepdims=True)
    norm = jnp.sqrt(jnp.broadcast_to(total, (8, 128)))
    clip[...] = jnp.minimum(1.0, 1.0 / (norm + CLIP_EPS))


def adamw(mean, master, exp_avg, exp_avg_sq, clip, decay):
    clipped = clip * mean
    avg_new = ADAM_BETA1 * exp_avg + (1.0 - ADAM_BETA1) * clipped
    sq_new = ADAM_BETA2 * exp_avg_sq + (1.0 - ADAM_BETA2) * clipped * clipped
    step_dir = (avg_new / BIAS_ONE) / (jnp.sqrt(sq_new / BIAS_TWO) + ADAM_EPS)
    master_new = master - LEARN_RATE * (step_dir + decay * master)
    return master_new, avg_new, sq_new, master_new.astype(jnp.bfloat16)


def update_kernel(*refs):
    means, states, clip_ref = refs[:4], refs[4:16], refs[16]
    outs, bufs, sem = refs[17:33], refs[33:49], refs[49]
    clip = clip_ref[...]

    def rows(array, index):
        ins = [means[array]] + list(states[3 * array:3 * array + 3])
        ins = [r[index] for r in ins]
        height, width = ins[0].shape
        scale = jnp.concatenate([clip[:height]] * -(-width // 128), axis=1)[:, :width]
        for o, value in zip(bufs[4 * array:4 * array + 4], adamw(*ins, scale, DECAYS[array])):
            o[index] = value

    def send(array, index):
        for k in range(4 * array, 4 * array + 4):
            pltpu.make_async_copy(at(bufs[k], index), at(outs[k], index), sem.at[k % SEMS]).start()

    for l in range(6):
        for r in range(0, 64, 8):
            rows(LAYER, (l, slice(r, r + 8)))
        send(LAYER, (l,))
    for r in range(0, 64, 8):
        rows(DOWN, (slice(r, r + 8),))
        send(DOWN, (slice(r, r + 8),))
    for r in range(0, 64, 8):
        rows(EMBED, (slice(r, r + 8),))
    send(EMBED, ())
    rows(NORM, (slice(0, 4),))
    send(NORM, ())
    for k in range(16):
        pltpu.make_async_copy(bufs[k], outs[k], sem.at[k % SEMS]).wait()


SEMS = 1


def solution(mesh):
    grad_four = P(("dp", "fsdp"), None, None, None)
    grad_three = P(("dp", "fsdp"), None, None)
    layer_spec = P(None, "fsdp", None)
    down_spec = P("fsdp", None)
    norm_spec = P(None, "fsdp")
    embed_spec = P("fsdp", None)
    any_spec = pl.BlockSpec(memory_space=pl.ANY)
    vmem_spec = pl.BlockSpec(memory_space=pltpu.VMEM)
    dma = pltpu.SemaphoreType.DMA
    f32 = jnp.float32

    def local_update(*args):
        state_shapes = [s for s in SHARES for _ in range(3)]
        results = pl.pallas_call(
            reduce_kernel,
            out_shape=tuple(pltpu.VMEM(s, f32) for s in list(SHARES) + state_shapes + [(8, 128)]),
            in_specs=[any_spec] * 16,
            out_specs=(vmem_spec,) * 17,
            scratch_shapes=[pltpu.VMEM(lead + s, f32) for lead in ((2,), (2,), (), ()) for s in WINDOWS] + [
                pltpu.VMEM((2, 8, 896), f32), pltpu.VMEM((4, 8, 128), f32), pltpu.VMEM((8, 128), f32),
                dma, dma((2, PAIR_RING)), dma, dma, dma, dma, dma((X_RING,)), dma((Y_RING,)), dma, dma((3,)),
            ],
            compiler_params=pltpu.CompilerParams(
                collective_id=0, has_side_effects=True, vmem_limit_bytes=24 * 1024 * 1024),
            name="reduce_grads",
        )(*(pltpu.with_memory_space_constraint(a, pltpu.HBM) for a in args))
        out_shapes = [(s, d) for s in SHARES for d in (f32, f32, f32, jnp.bfloat16)]
        return pl.pallas_call(
            update_kernel,
            out_shape=tuple(jax.ShapeDtypeStruct(s, d) for s, d in out_shapes),
            in_specs=[vmem_spec] * 17,
            out_specs=(any_spec,) * 16,
            scratch_shapes=[pltpu.VMEM(s, d) for s, d in out_shapes] + [dma((SEMS,))],
            compiler_params=pltpu.CompilerParams(vmem_limit_bytes=16 * 1024 * 1024),
            name="adamw_update",
        )(*(pltpu.with_memory_space_constraint(r, pltpu.VMEM) for r in results))

    in_specs = (grad_four, grad_three, grad_three, grad_three,
                layer_spec, layer_spec, layer_spec, down_spec, down_spec, down_spec,
                norm_spec, norm_spec, norm_spec, embed_spec, embed_spec, embed_spec)
    out_specs = (layer_spec,) * 4 + (down_spec,) * 4 + (norm_spec,) * 4 + (embed_spec,) * 4
    return jax.shard_map(local_update, mesh=mesh, in_specs=in_specs, out_specs=out_specs, check_vma=False)
```

```python
import jax
import jax.numpy as jnp
from jax import lax
from jax.experimental import pallas as pl
from jax.experimental.pallas import tpu as pltpu
from jax.sharding import PartitionSpec as P

ADAM_BETA1 = 0.9
ADAM_BETA2 = 0.95
ADAM_EPS = 1e-8
LEARN_RATE = 4e-4
WEIGHT_DECAY = 0.1
CLIP_EPS = 1e-6
OPT_STEP = 20
BIAS_ONE = 1.0 - ADAM_BETA1 ** OPT_STEP
BIAS_TWO = 1.0 - ADAM_BETA2 ** OPT_STEP

MESH = pl.DeviceIdType.MESH
LAYER, DOWN, NORM, EMBED = range(4)
DECAYS = (WEIGHT_DECAY, WEIGHT_DECAY, WEIGHT_DECAY, 0.0)
SHARES = ((6, 64, 896), (64, 4864), (4, 224), (64, 896))
WINDOWS = ((6, 64, 896), (64, 4864), (4, 384), (64, 896))
EARLY = 32
HALF = EARLY // 2
PIECES = range(0, HALF, 8)

GROUPS = ([(EMBED, None, slice(EARLY, EARLY + 8)), (EMBED, None, slice(0, EARLY)), (EMBED, None, slice(EARLY + 8, 64)),
           (LAYER, 0, None), (NORM, None, None)]
          + [(DOWN, None, slice(r, r + 8)) for r in range(0, 64, 8)] + [(LAYER, l, None) for l in range(1, 6)])
STAGED = 4
PAIR_AHEAD = 4
PAIR_RING = 2 * PAIR_AHEAD


def plan():
    chunks = [(EMBED, (slice(r, r + 8),), 0 if r == EARLY else 2) for r in range(EARLY, 64, 8)]
    chunks += [(LAYER, (0, slice(r, r + 8)), 3) for r in range(0, 64, 8)]
    chunks.append((NORM, (), 4))
    cuts = (0, 1024, 2048, 3072, 3968, 4864)
    chunks += [(DOWN, (slice(r, r + 8), slice(a, b)), 5 + r // 8) for r in range(0, 64, 8) for a, b in zip(cuts, cuts[1:])]
    chunks += [(LAYER, (l, slice(r, r + 8)), 12 + l) for l in range(1, 6) for r in range(0, 64, 8)]
    return chunks


CHUNKS = plan()
X_AHEAD, Y_BEHIND = 8, 5
X_RING, Y_RING = 2 * X_AHEAD + 2, 2 * Y_BEHIND + 2
EARLY_STEPS = {11: 0, 15: 1}


def at(ref, index):
    return ref.at[tuple(pl.ds(i.start, i.stop - i.start) if isinstance(i, slice) else i for i in index)] if index else ref


def tile_sum(value):
    rows, columns = value.shape
    parts = [value[r:r + 8, c:c + 128] for r in range(0, rows, 8) for c in range(0, columns, 128)]
    while len(parts) > 1:
        parts = [a + b for a, b in zip(parts[::2], parts[1::2])] + parts[len(parts) // 2 * 2:]
    return parts[0]


def reduce_kernel(*refs):
    grads, states = refs[:4], refs[4:16]
    means, copies, clip = refs[16:20], refs[20:32], refs[32]
    far, near, x_in, y_in = (refs[33 + 4 * i:37 + 4 * i] for i in range(4))
    (first, early_in, norms, acc, first_sem, group_sem, state_sem, pair_send, x_send, y_send, x_recv, y_recv,
     early_recv, early_x, early_y, norm_send, norm_recv) = refs[49:]

    dp, me = lax.axis_index("dp"), lax.axis_index("fsdp")
    partner = me + 1 - 2 * lax.rem(me, 2)
    across = lax.rem(me + 2, 4)
    diagonal = lax.rem(partner + 2, 4)
    other = 1 - dp
    peers = ((dp, across), (dp, diagonal), (dp, partner))
    held = (far, near)

    def share(array, fsdp, layer=None, rows=None):
        ref = grads[array].at[0]
        if array == NORM:
            start = jnp.minimum((fsdp * 7) // 4, 4)
            return ref.at[:, pl.ds(pl.multiple_of(start * 128, 128), 384)]
        rows = rows or slice(0, 64)
        window = pl.ds(pl.multiple_of(fsdp * 64 + rows.start, 8), rows.stop - rows.start)
        return ref.at[layer, window, :] if array == LAYER else ref.at[window, :]

    def slot(which, g, i):
        array, layer, rows = GROUPS[g]
        ref = held[which][array]
        lead = i if i is not None else slice(0, 2)
        return at(ref, (lead, layer) if array == LAYER else (lead, rows) if rows is not None else (lead,))

    def load(which, g):
        array, layer, rows = GROUPS[g]
        return pltpu.make_async_copy(
            share(array, (across, me)[which], layer, rows), slot(which, g, 0), group_sem.at[which, g % PAIR_RING])

    def stage(which, i):
        return pltpu.make_async_copy(
            share((EMBED, LAYER)[i], (diagonal, partner)[which], 0), first.at[i, which], first_sem.at[i])

    def pair(which, g):
        array, layer, rows = GROUPS[g]
        return pltpu.make_async_remote_copy(
            src_ref=share(array, (diagonal, partner)[which], layer, rows) if g >= STAGED else at(first, (int(array == LAYER), which) + (() if rows is None else (rows,))),
            dst_ref=slot(which, g, 1), send_sem=pair_send, recv_sem=group_sem.at[which, g % PAIR_RING],
            device_id=(dp, partner), device_id_type=MESH)

    def over_x(c):
        array, index, _ = CHUNKS[c]
        return pltpu.make_async_remote_copy(
            src_ref=at(far[array].at[0], index), dst_ref=at(x_in[array], index),
            send_sem=x_send, recv_sem=x_recv.at[c % X_RING], device_id=(dp, across), device_id_type=MESH)

    def over_y(c):
        array, index, _ = CHUNKS[c]
        return pltpu.make_async_remote_copy(
            src_ref=at(near[array].at[0], index), dst_ref=at(y_in[array], index),
            send_sem=y_send, recv_sem=y_recv.at[c % Y_RING], device_id=(other, me), device_id_type=MESH)

    def half(owner, piece=None):
        start, size = (0, HALF) if piece is None else (PIECES[piece], 8)
        return pl.ds(pl.multiple_of(owner * HALF + start, 8), size)

    def early(which):
        return pltpu.make_async_remote_copy(
            src_ref=held[which][EMBED].at[0, half(other), :], dst_ref=early_in.at[which],
            send_sem=y_send, recv_sem=early_recv.at[which], device_id=(other, me), device_id_type=MESH)

    def early_over_x(piece):
        return pltpu.make_async_remote_copy(
            src_ref=far[EMBED].at[0, half(dp, piece), :], dst_ref=x_in[EMBED].at[half(dp, piece), :],
            send_sem=x_send, recv_sem=early_x.at[piece], device_id=(dp, across), device_id_type=MESH)

    def early_over_y(piece, owner):
        return pltpu.make_async_remote_copy(
            src_ref=near[EMBED].at[0, half(owner, piece), :], dst_ref=y_in[EMBED].at[half(owner, piece), :],
            send_sem=y_send, recv_sem=early_y.at[piece], device_id=(other, me), device_id_type=MESH)

    def norm_to(i):
        return pltpu.make_async_remote_copy(
            src_ref=norms.at[me], dst_ref=norms.at[me], send_sem=norm_send, recv_sem=norm_recv.at[i],
            device_id=peers[i], device_id_type=MESH)

    barrier = pltpu.get_barrier_semaphore()
    for device in ((other, me),) + peers:
        pl.semaphore_signal(barrier, inc=1, device_id=device, device_id_type=MESH)
    for i in (0, 1):
        for which in (0, 1):
            stage(which, i).start()
    for g in range(PAIR_AHEAD):
        for which in (0, 1):
            load(which, g).start()
    acc[...] = jnp.zeros_like(acc)
    pltpu.make_async_copy(first.at[0], first.at[0], first_sem.at[0]).wait()
    pl.semaphore_wait(barrier, 4)
    for which, g in ((0, 0), (0, 1), (0, 2), (1, 1), (1, 0), (1, 2)):
        pair(which, g).start()
    pltpu.make_async_copy(first.at[1], first.at[1], first_sem.at[1]).wait()
    for which in (0, 1):
        pair(which, 3).start()
    for s, d in zip(states, copies):
        pltpu.make_async_copy(s, d, state_sem).start()

    ready = set()

    def need(which, g):
        if (which, g) not in ready:
            ready.add((which, g))
            ref = slot(which, g, None)
            pltpu.make_async_copy(ref, ref, group_sem.at[which, g % PAIR_RING]).wait()
            if g + PAIR_AHEAD < len(GROUPS):
                pair(which, g + PAIR_AHEAD).start()
                load(which, g + PAIR_AHEAD).start()

    def send_x(c):
        array, index, g = CHUNKS[c]
        need(0, g)
        ref = at(far[array].at[0], index)
        ref[...] = ref[...] + at(far[array].at[1], index)[...]
        over_x(c).start()

    def send_y(c):
        array, index, g = CHUNKS[c]
        need(1, g)
        over_x(c).wait_recv()
        ref = at(near[array].at[0], index)
        ref[...] = (ref[...] + at(near[array].at[1], index)[...]) + at(x_in[array], index)[...]
        over_y(c).start()

    def finish(c):
        array, index, _ = CHUNKS[c]
        over_y(c).wait_recv()
        mean = (at(near[array].at[0], index)[...] + at(y_in[array], index)[...]) * (1.0 / 8.0)
        if array == NORM:
            for f, skip in enumerate((0, 96, 64, 160)):
                @pl.when(me == f)
                def _():
                    mine = pltpu.roll(mean, (384 - skip) % 384, axis=1)
                    mine = jnp.where(lax.broadcasted_iota(jnp.int32, (4, 384), 1) < 224, mine, 0.0)
                    means[NORM][...] = mine[:, :224]
                    square = mine * mine
                    acc[0:4, :] = acc[0:4, :] + (square[:, :128] + square[:, 128:256])
        else:
            at(means[array], index)[...] = mean
            total = acc[...] + tile_sum(mean * mean)
            if c < len(CHUNKS) - 1:
                acc[...] = total
            else:
                norms[me] = total

    def send_early(which):
        need(which, 1)
        ref = held[which][EMBED]
        for owner in (other, dp):
            ref[0, half(owner), :] = ref[0, half(owner), :] + ref[1, half(owner), :]
            if owner is other:
                early(which).start()

    def send_early_x(piece):
        if piece == 0:
            early(0).wait_recv()
        rows = half(dp, piece)
        far[EMBED][0, rows, :] = far[EMBED][0, rows, :] + early_in[0, PIECES[piece]:PIECES[piece] + 8, :]
        early_over_x(piece).start()

    def send_early_y(piece):
        if piece == 0:
            early(1).wait_recv()
        early_over_x(piece).wait_recv()
        rows = half(dp, piece)
        total = (near[EMBED][0, rows, :] + early_in[1, PIECES[piece]:PIECES[piece] + 8, :]) + x_in[EMBED][rows, :]
        near[EMBED][0, rows, :] = total
        means[EMBED][rows, :] = total * (1.0 / 8.0)
        early_over_y(piece, dp).start()

    def finish_early(piece):
        early_over_y(piece, other).wait_recv()
        rows = half(other, piece)
        means[EMBED][rows, :] = y_in[EMBED][rows, :] * (1.0 / 8.0)
        total = acc[...]
        for owner in (0, 1):
            mean = means[EMBED][half(owner, piece), :]
            total = total + tile_sum(mean * mean)
        acc[...] = total

    count = len(CHUNKS)
    for step in range(count + X_AHEAD + Y_BEHIND):
        if step < count:
            send_x(step)
        if step == 0:
            send_early(0)
            send_early(1)

            @pl.when(lax.rem(me, 2) == 1)
            def _():
                pl.delay(1800)
        if step in EARLY_STEPS:
            send_early_x(EARLY_STEPS[step])
        if 0 <= step - X_AHEAD < count:
            send_y(step - X_AHEAD)
        if step - X_AHEAD in EARLY_STEPS:
            send_early_y(EARLY_STEPS[step - X_AHEAD])
        if 0 <= step - X_AHEAD - Y_BEHIND < count:
            finish(step - X_AHEAD - Y_BEHIND)
        if step - X_AHEAD - Y_BEHIND in EARLY_STEPS:
            finish_early(EARLY_STEPS[step - X_AHEAD - Y_BEHIND])
    for i in range(3):
        norm_to(i).start()

    for s, d in zip(states, copies):
        pltpu.make_async_copy(s, d, state_sem).wait()
    for array in range(4):
        for which in (0, 1):
            ref = held[which][array].at[0]
            pltpu.make_async_remote_copy(
                src_ref=ref, dst_ref=ref, send_sem=pair_send, recv_sem=norm_recv.at[0],
                device_id=(dp, partner), device_id_type=MESH).wait_send()
        rows = slice(HALF, 64) if array == EMBED else None
        index = () if rows is None else (rows,)
        pltpu.make_async_remote_copy(
            src_ref=at(far[array].at[0], index), dst_ref=at(x_in[array], index), send_sem=x_send, recv_sem=norm_recv.at[0],
            device_id=(dp, across), device_id_type=MESH).wait_send()
        pltpu.make_async_remote_copy(
            src_ref=near[array].at[0], dst_ref=y_in[array], send_sem=y_send, recv_sem=norm_recv.at[0],
            device_id=(other, me), device_id_type=MESH).wait_send()
    early(0).wait_send()
    for i in range(3):
        norm_to(i).wait_send()
    for i in range(3):
        norm_to(i).wait_recv()
    total = (norms[0] + norms[1]) + (norms[2] + norms[3])
    total = jnp.sum(jnp.sum(total, axis=0, keepdims=True), axis=1, keepdims=True)
    norm = jnp.sqrt(jnp.broadcast_to(total, (8, 128)))
    clip[...] = jnp.minimum(1.0, 1.0 / (norm + CLIP_EPS))


def adamw(mean, master, exp_avg, exp_avg_sq, clip, decay):
    clipped = clip * mean
    avg_new = ADAM_BETA1 * exp_avg + (1.0 - ADAM_BETA1) * clipped
    sq_new = ADAM_BETA2 * exp_avg_sq + (1.0 - ADAM_BETA2) * clipped * clipped
    step_dir = (avg_new / BIAS_ONE) / (jnp.sqrt(sq_new / BIAS_TWO) + ADAM_EPS)
    master_new = master - LEARN_RATE * (step_dir + decay * master)
    return master_new, avg_new, sq_new, master_new.astype(jnp.bfloat16)


def update_kernel(*refs):
    means, states, clip_ref = refs[:4], refs[4:16], refs[16]
    outs, bufs, sem = refs[17:33], refs[33:49], refs[49]
    clip = clip_ref[...]

    def rows(array, index):
        ins = [means[array]] + list(states[3 * array:3 * array + 3])
        ins = [r[index] for r in ins]
        height, width = ins[0].shape
        scale = jnp.concatenate([clip[:height]] * -(-width // 128), axis=1)[:, :width]
        for o, value in zip(bufs[4 * array:4 * array + 4], adamw(*ins, scale, DECAYS[array])):
            o[index] = value

    def send(array, index):
        for k in range(4 * array, 4 * array + 4):
            pltpu.make_async_copy(at(bufs[k], index), at(outs[k], index), sem.at[k % SEMS]).start()

    for l in range(6):
        for r in range(0, 64, 8):
            rows(LAYER, (l, slice(r, r + 8)))
        send(LAYER, (l,))
    for r in range(0, 64, 8):
        rows(DOWN, (slice(r, r + 8),))
        send(DOWN, (slice(r, r + 8),))
    for r in range(0, 64, 8):
        rows(EMBED, (slice(r, r + 8),))
    send(EMBED, ())
    rows(NORM, (slice(0, 4),))
    send(NORM, ())
    for k in range(16):
        pltpu.make_async_copy(bufs[k], outs[k], sem.at[k % SEMS]).wait()


SEMS = 1


def solution(mesh):
    grad_four = P(("dp", "fsdp"), None, None, None)
    grad_three = P(("dp", "fsdp"), None, None)
    layer_spec = P(None, "fsdp", None)
    down_spec = P("fsdp", None)
    norm_spec = P(None, "fsdp")
    embed_spec = P("fsdp", None)
    any_spec = pl.BlockSpec(memory_space=pl.ANY)
    vmem_spec = pl.BlockSpec(memory_space=pltpu.VMEM)
    dma = pltpu.SemaphoreType.DMA
    f32 = jnp.float32

    def local_update(*args):
        state_shapes = [s for s in SHARES for _ in range(3)]
        results = pl.pallas_call(
            reduce_kernel,
            out_shape=tuple(pltpu.VMEM(s, f32) for s in list(SHARES) + state_shapes + [(8, 128)]),
            in_specs=[any_spec] * 16,
            out_specs=(vmem_spec,) * 17,
            scratch_shapes=[pltpu.VMEM(lead + s, f32) for lead in ((2,), (2,), (), ()) for s in WINDOWS] + [
                pltpu.VMEM((2, 2, 64, 896), f32), pltpu.VMEM((2, HALF, 896), f32), pltpu.VMEM((4, 8, 128), f32), pltpu.VMEM((8, 128), f32),
                dma((2,)), dma((2, PAIR_RING)), dma, dma, dma, dma, dma((X_RING,)), dma((Y_RING,)),
                dma((2,)), dma((len(PIECES),)), dma((len(PIECES),)), dma, dma((3,)),
            ],
            compiler_params=pltpu.CompilerParams(
                collective_id=0, has_side_effects=True, vmem_limit_bytes=24 * 1024 * 1024),
            name="reduce_grads",
        )(*(pltpu.with_memory_space_constraint(a, pltpu.HBM) for a in args))
        out_shapes = [(s, d) for s in SHARES for d in (f32, f32, f32, jnp.bfloat16)]
        return pl.pallas_call(
            update_kernel,
            out_shape=tuple(jax.ShapeDtypeStruct(s, d) for s, d in out_shapes),
            in_specs=[vmem_spec] * 17,
            out_specs=(any_spec,) * 16,
            scratch_shapes=[pltpu.VMEM(s, d) for s, d in out_shapes] + [dma((SEMS,))],
            compiler_params=pltpu.CompilerParams(vmem_limit_bytes=16 * 1024 * 1024),
            name="adamw_update",
        )(*(pltpu.with_memory_space_constraint(r, pltpu.VMEM) for r in results))

    in_specs = (grad_four, grad_three, grad_three, grad_three,
                layer_spec, layer_spec, layer_spec, down_spec, down_spec, down_spec,
                norm_spec, norm_spec, norm_spec, embed_spec, embed_spec, embed_spec)
    out_specs = (layer_spec,) * 4 + (down_spec,) * 4 + (norm_spec,) * 4 + (embed_spec,) * 4
    return jax.shard_map(local_update, mesh=mesh, in_specs=in_specs, out_specs=out_specs, check_vma=False)
```

```python
import jax
import jax.numpy as jnp
from jax import lax
from jax.experimental import pallas as pl
from jax.experimental.pallas import tpu as pltpu
from jax.sharding import PartitionSpec as P

ADAM_BETA1 = 0.9
ADAM_BETA2 = 0.95
ADAM_EPS = 1e-8
LEARN_RATE = 4e-4
WEIGHT_DECAY = 0.1
CLIP_EPS = 1e-6
OPT_STEP = 20
BIAS_ONE = 1.0 - ADAM_BETA1 ** OPT_STEP
BIAS_TWO = 1.0 - ADAM_BETA2 ** OPT_STEP

MESH = pl.DeviceIdType.MESH
LAYER, DOWN, NORM, EMBED = range(4)
DECAYS = (WEIGHT_DECAY, WEIGHT_DECAY, WEIGHT_DECAY, 0.0)
SHARES = ((6, 64, 896), (64, 4864), (4, 224), (64, 896))
WINDOWS = ((6, 64, 896), (64, 4864), (4, 384), (64, 896))
EARLY = 32
HALF = EARLY // 2
PIECES = range(0, HALF, 8)

GROUPS = ([(EMBED, None, slice(EARLY, EARLY + 8)), (EMBED, None, slice(0, EARLY)), (EMBED, None, slice(EARLY + 8, 64)),
           (LAYER, 0, None), (NORM, None, None)]
          + [(DOWN, None, slice(r, r + 8)) for r in range(0, 64, 8)] + [(LAYER, l, None) for l in range(1, 6)])
STAGED = 4
PAIR_AHEAD = 4
PAIR_RING = 2 * PAIR_AHEAD


def plan():
    chunks = [(EMBED, (slice(r, r + 8),), 0 if r == EARLY else 2) for r in range(EARLY, 64, 8)]
    chunks += [(LAYER, (0, slice(r, r + 8)), 3) for r in range(0, 64, 8)]
    chunks.append((NORM, (), 4))
    cuts = (0, 1024, 2048, 3072, 3968, 4864)
    chunks += [(DOWN, (slice(r, r + 8), slice(a, b)), 5 + r // 8) for r in range(0, 64, 8) for a, b in zip(cuts, cuts[1:])]
    chunks += [(LAYER, (l, slice(r, r + 8)), 12 + l) for l in range(1, 6) for r in range(0, 64, 8)]
    return chunks


CHUNKS = plan()
X_AHEAD, Y_BEHIND = 6, 5
X_RING, Y_RING = 2 * X_AHEAD + 2, 2 * Y_BEHIND + 2
EARLY_STEPS = {11: 0, 15: 1}


def at(ref, index):
    return ref.at[tuple(pl.ds(i.start, i.stop - i.start) if isinstance(i, slice) else i for i in index)] if index else ref


def tile_sum(value):
    rows, columns = value.shape
    parts = [value[r:r + 8, c:c + 128] for r in range(0, rows, 8) for c in range(0, columns, 128)]
    while len(parts) > 1:
        parts = [a + b for a, b in zip(parts[::2], parts[1::2])] + parts[len(parts) // 2 * 2:]
    return parts[0]


def reduce_kernel(*refs):
    grads, states = refs[:4], refs[4:16]
    means, copies, clip = refs[16:20], refs[20:32], refs[32]
    far, near, x_in, y_in = (refs[33 + 4 * i:37 + 4 * i] for i in range(4))
    (first, raw_in, early_in, norms, acc, first_sem, group_sem, state_sem, send_sem, x_recv, y_recv,
     early_recv, early_x, early_y, raw_recv, norm_recv) = refs[49:]

    dp, me = lax.axis_index("dp"), lax.axis_index("fsdp")
    partner = me + 1 - 2 * lax.rem(me, 2)
    across = lax.rem(me + 2, 4)
    diagonal = lax.rem(partner + 2, 4)
    other = 1 - dp
    peers = ((dp, across), (dp, diagonal), (dp, partner))
    held = (far, near)

    def share(array, fsdp, layer=None, rows=None):
        ref = grads[array].at[0]
        if array == NORM:
            start = jnp.minimum((fsdp * 7) // 4, 4)
            return ref.at[:, pl.ds(pl.multiple_of(start * 128, 128), 384)]
        rows = rows or slice(0, 64)
        window = pl.ds(pl.multiple_of(fsdp * 64 + rows.start, 8), rows.stop - rows.start)
        return ref.at[layer, window, :] if array == LAYER else ref.at[window, :]

    def slot(which, g, i):
        array, layer, rows = GROUPS[g]
        ref = held[which][array]
        lead = i if i is not None else slice(0, 2)
        return at(ref, (lead, layer) if array == LAYER else (lead, rows) if rows is not None else (lead,))

    def load(which, g):
        array, layer, rows = GROUPS[g]
        return pltpu.make_async_copy(
            share(array, (across, me)[which], layer, rows), slot(which, g, 0), group_sem.at[which, g % PAIR_RING])

    def stage(which, i):
        return pltpu.make_async_copy(
            share((EMBED, LAYER)[i], (diagonal, partner)[which], 0), first.at[i, which], first_sem.at[i])

    def pair(which, g):
        array, layer, rows = GROUPS[g]
        return pltpu.make_async_remote_copy(
            src_ref=share(array, (diagonal, partner)[which], layer, rows) if g >= STAGED else at(first, (int(array == LAYER), which) + (() if rows is None else (rows,))),
            dst_ref=slot(which, g, 1), send_sem=send_sem, recv_sem=group_sem.at[which, g % PAIR_RING],
            device_id=(dp, partner), device_id_type=MESH)

    def over_x(c):
        array, index, _ = CHUNKS[c]
        return pltpu.make_async_remote_copy(
            src_ref=at(far[array].at[0], index), dst_ref=at(x_in[array], index),
            send_sem=send_sem, recv_sem=x_recv.at[c % X_RING], device_id=(dp, across), device_id_type=MESH)

    def raw():
        return pltpu.make_async_remote_copy(
            src_ref=first.at[0, 0, pl.ds(EARLY, 8), :], dst_ref=raw_in, send_sem=send_sem, recv_sem=raw_recv,
            device_id=(dp, diagonal), device_id_type=MESH)

    def over_y(c):
        array, index, _ = CHUNKS[c]
        return pltpu.make_async_remote_copy(
            src_ref=at(near[array].at[0], index), dst_ref=at(y_in[array], index),
            send_sem=send_sem, recv_sem=y_recv.at[c % Y_RING], device_id=(other, me), device_id_type=MESH)

    def half(owner, piece=None):
        start, size = (0, HALF) if piece is None else (PIECES[piece], 8)
        return pl.ds(pl.multiple_of(owner * HALF + start, 8), size)

    def early(which):
        return pltpu.make_async_remote_copy(
            src_ref=held[which][EMBED].at[0, half(other), :], dst_ref=early_in.at[which],
            send_sem=send_sem, recv_sem=early_recv.at[which], device_id=(other, me), device_id_type=MESH)

    def early_over_x(piece):
        return pltpu.make_async_remote_copy(
            src_ref=far[EMBED].at[0, half(dp, piece), :], dst_ref=x_in[EMBED].at[half(dp, piece), :],
            send_sem=send_sem, recv_sem=early_x.at[piece], device_id=(dp, across), device_id_type=MESH)

    def early_over_y(piece, owner):
        return pltpu.make_async_remote_copy(
            src_ref=near[EMBED].at[0, half(owner, piece), :], dst_ref=y_in[EMBED].at[half(owner, piece), :],
            send_sem=send_sem, recv_sem=early_y.at[piece], device_id=(other, me), device_id_type=MESH)

    def norm_to(i):
        return pltpu.make_async_remote_copy(
            src_ref=norms.at[me], dst_ref=norms.at[me], send_sem=send_sem, recv_sem=norm_recv.at[i],
            device_id=peers[i], device_id_type=MESH)

    barrier = pltpu.get_barrier_semaphore()
    for device in ((other, me),) + peers:
        pl.semaphore_signal(barrier, inc=1, device_id=device, device_id_type=MESH)
    for i in (0, 1):
        for which in (0, 1):
            stage(which, i).start()
    for g in range(PAIR_AHEAD):
        for which in (0, 1):
            load(which, g).start()
    acc[...] = jnp.zeros_like(acc)
    pltpu.make_async_copy(first.at[0], first.at[0], first_sem.at[0]).wait()
    pl.semaphore_wait(barrier, 4)
    ready = set()

    def need(which, g):
        if (which, g) not in ready:
            ready.add((which, g))
            ref = slot(which, g, None if (which, g) != (0, 0) else 0)
            pltpu.make_async_copy(ref, ref, group_sem.at[which, g % PAIR_RING]).wait()
            if g + PAIR_AHEAD < len(GROUPS):
                pair(which, g + PAIR_AHEAD).start()
                load(which, g + PAIR_AHEAD).start()

    need(0, 0)
    over_x(0).start()
    raw().start()
    for which, g in ((0, 1), (0, 2), (1, 1), (1, 0), (1, 2)):
        pair(which, g).start()
    pltpu.make_async_copy(first.at[1], first.at[1], first_sem.at[1]).wait()
    for which in (0, 1):
        pair(which, 3).start()
    for s, d in zip(states, copies):
        pltpu.make_async_copy(s, d, state_sem).start()


    def send_x(c):
        if c == 0:
            return
        array, index, g = CHUNKS[c]
        need(0, g)
        ref = at(far[array].at[0], index)
        ref[...] = ref[...] + at(far[array].at[1], index)[...]
        over_x(c).start()

    def send_y(c):
        array, index, g = CHUNKS[c]
        need(1, g)
        over_x(c).wait_recv()
        ref = at(near[array].at[0], index)
        total = (ref[...] + at(near[array].at[1], index)[...]) + at(x_in[array], index)[...]
        if c == 0:
            raw().wait_recv()
            total = total + raw_in[...]
        ref[...] = total
        over_y(c).start()

    def finish(c):
        array, index, _ = CHUNKS[c]
        over_y(c).wait_recv()
        mean = (at(near[array].at[0], index)[...] + at(y_in[array], index)[...]) * (1.0 / 8.0)
        if array == NORM:
            for f, skip in enumerate((0, 96, 64, 160)):
                @pl.when(me == f)
                def _():
                    mine = pltpu.roll(mean, (384 - skip) % 384, axis=1)
                    mine = jnp.where(lax.broadcasted_iota(jnp.int32, (4, 384), 1) < 224, mine, 0.0)
                    means[NORM][...] = mine[:, :224]
                    square = mine * mine
                    acc[0:4, :] = acc[0:4, :] + (square[:, :128] + square[:, 128:256])
        else:
            at(means[array], index)[...] = mean
            total = acc[...] + tile_sum(mean * mean)
            if c < len(CHUNKS) - 1:
                acc[...] = total
            else:
                norms[me] = total

    def send_early(which):
        need(which, 1)
        ref = held[which][EMBED]
        for owner in (other, dp):
            ref[0, half(owner), :] = ref[0, half(owner), :] + ref[1, half(owner), :]
            if owner is other:
                early(which).start()

    def send_early_x(piece):
        if piece == 0:
            early(0).wait_recv()
        rows = half(dp, piece)
        far[EMBED][0, rows, :] = far[EMBED][0, rows, :] + early_in[0, PIECES[piece]:PIECES[piece] + 8, :]
        early_over_x(piece).start()

    def send_early_y(piece):
        if piece == 0:
            early(1).wait_recv()
        early_over_x(piece).wait_recv()
        rows = half(dp, piece)
        total = (near[EMBED][0, rows, :] + early_in[1, PIECES[piece]:PIECES[piece] + 8, :]) + x_in[EMBED][rows, :]
        near[EMBED][0, rows, :] = total
        means[EMBED][rows, :] = total * (1.0 / 8.0)
        early_over_y(piece, dp).start()

    def finish_early(piece):
        early_over_y(piece, other).wait_recv()
        rows = half(other, piece)
        means[EMBED][rows, :] = y_in[EMBED][rows, :] * (1.0 / 8.0)
        total = acc[...]
        for owner in (0, 1):
            mean = means[EMBED][half(owner, piece), :]
            total = total + tile_sum(mean * mean)
        acc[...] = total

    count = len(CHUNKS)
    for step in range(count + X_AHEAD + Y_BEHIND):
        if step < count:
            send_x(step)
        if step == 0:
            send_early(0)
            send_early(1)

            @pl.when(lax.rem(me, 2) == 1)
            def _():
                pl.delay(1800)
        if step in EARLY_STEPS:
            send_early_x(EARLY_STEPS[step])
        if 0 <= step - X_AHEAD < count:
            send_y(step - X_AHEAD)
        if step - X_AHEAD in EARLY_STEPS:
            send_early_y(EARLY_STEPS[step - X_AHEAD])
        if 0 <= step - X_AHEAD - Y_BEHIND < count:
            finish(step - X_AHEAD - Y_BEHIND)
        if step - X_AHEAD - Y_BEHIND in EARLY_STEPS:
            finish_early(EARLY_STEPS[step - X_AHEAD - Y_BEHIND])
    for i in range(3):
        norm_to(i).start()

    for s, d in zip(states, copies):
        pltpu.make_async_copy(s, d, state_sem).wait()
    for array in range(4):
        for which in (0, 1):
            ref = held[which][array].at[0]
            pltpu.make_async_remote_copy(
                src_ref=ref, dst_ref=ref, send_sem=send_sem, recv_sem=norm_recv.at[0],
                device_id=(dp, partner), device_id_type=MESH).wait_send()
        rows = slice(HALF, 64) if array == EMBED else None
        index = () if rows is None else (rows,)
        pltpu.make_async_remote_copy(
            src_ref=at(far[array].at[0], index), dst_ref=at(x_in[array], index), send_sem=send_sem, recv_sem=norm_recv.at[0],
            device_id=(dp, across), device_id_type=MESH).wait_send()
        pltpu.make_async_remote_copy(
            src_ref=near[array].at[0], dst_ref=y_in[array], send_sem=send_sem, recv_sem=norm_recv.at[0],
            device_id=(other, me), device_id_type=MESH).wait_send()
    early(0).wait_send()
    for i in range(3):
        norm_to(i).wait_send()
    for i in range(3):
        norm_to(i).wait_recv()
    total = (norms[0] + norms[1]) + (norms[2] + norms[3])
    total = jnp.sum(jnp.sum(total, axis=0, keepdims=True), axis=1, keepdims=True)
    norm = jnp.sqrt(jnp.broadcast_to(total, (8, 128)))
    clip[...] = jnp.minimum(1.0, 1.0 / (norm + CLIP_EPS))


def adamw(mean, master, exp_avg, exp_avg_sq, clip, decay):
    clipped = clip * mean
    avg_new = ADAM_BETA1 * exp_avg + (1.0 - ADAM_BETA1) * clipped
    sq_new = ADAM_BETA2 * exp_avg_sq + (1.0 - ADAM_BETA2) * clipped * clipped
    step_dir = (avg_new / BIAS_ONE) / (jnp.sqrt(sq_new / BIAS_TWO) + ADAM_EPS)
    master_new = master - LEARN_RATE * (step_dir + decay * master)
    return master_new, avg_new, sq_new, master_new.astype(jnp.bfloat16)


def update_kernel(*refs):
    means, states, clip_ref = refs[:4], refs[4:16], refs[16]
    outs, bufs, sem = refs[17:33], refs[33:49], refs[49]
    clip = clip_ref[...]

    def rows(array, index):
        ins = [means[array]] + list(states[3 * array:3 * array + 3])
        ins = [r[index] for r in ins]
        height, width = ins[0].shape
        scale = jnp.concatenate([clip[:height]] * -(-width // 128), axis=1)[:, :width]
        for o, value in zip(bufs[4 * array:4 * array + 4], adamw(*ins, scale, DECAYS[array])):
            o[index] = value

    def send(array, index):
        for k in range(4 * array, 4 * array + 4):
            pltpu.make_async_copy(at(bufs[k], index), at(outs[k], index), sem.at[k % SEMS]).start()

    for r in range(0, 64, 8):
        rows(LAYER, (0, slice(r, r + 8)))
        if r % 16:
            send(LAYER, (0, slice(r - 8, r + 8)))
    for l in range(1, 6):
        for r in range(0, 64, 8):
            rows(LAYER, (l, slice(r, r + 8)))
        send(LAYER, (l,))
    for r in range(0, 64, 8):
        rows(DOWN, (slice(r, r + 8),))
        send(DOWN, (slice(r, r + 8),))
    for r in range(0, 64, 8):
        rows(EMBED, (slice(r, r + 8),))
    send(EMBED, ())
    rows(NORM, (slice(0, 4),))
    send(NORM, ())
    for k in range(16):
        pltpu.make_async_copy(bufs[k], outs[k], sem.at[k % SEMS]).wait()


SEMS = 1


def solution(mesh):
    grad_four = P(("dp", "fsdp"), None, None, None)
    grad_three = P(("dp", "fsdp"), None, None)
    layer_spec = P(None, "fsdp", None)
    down_spec = P("fsdp", None)
    norm_spec = P(None, "fsdp")
    embed_spec = P("fsdp", None)
    any_spec = pl.BlockSpec(memory_space=pl.ANY)
    vmem_spec = pl.BlockSpec(memory_space=pltpu.VMEM)
    dma = pltpu.SemaphoreType.DMA
    f32 = jnp.float32

    def local_update(*args):
        state_shapes = [s for s in SHARES for _ in range(3)]
        results = pl.pallas_call(
            reduce_kernel,
            out_shape=tuple(pltpu.VMEM(s, f32) for s in list(SHARES) + state_shapes + [(8, 128)]),
            in_specs=[any_spec] * 16,
            out_specs=(vmem_spec,) * 17,
            scratch_shapes=[pltpu.VMEM(lead + s, f32) for lead in ((2,), (2,), (), ()) for s in WINDOWS] + [
                pltpu.VMEM((2, 2, 64, 896), f32), pltpu.VMEM((8, 896), f32), pltpu.VMEM((2, HALF, 896), f32), pltpu.VMEM((4, 8, 128), f32), pltpu.VMEM((8, 128), f32),
                dma((2,)), dma((2, PAIR_RING)), dma, dma, dma((X_RING,)), dma((Y_RING,)),
                dma((2,)), dma((len(PIECES),)), dma((len(PIECES),)), dma, dma((3,)),
            ],
            compiler_params=pltpu.CompilerParams(
                collective_id=0, has_side_effects=True, vmem_limit_bytes=24 * 1024 * 1024),
            name="reduce_grads",
        )(*(pltpu.with_memory_space_constraint(a, pltpu.HBM) for a in args))
        out_shapes = [(s, d) for s in SHARES for d in (f32, f32, f32, jnp.bfloat16)]
        return pl.pallas_call(
            update_kernel,
            out_shape=tuple(jax.ShapeDtypeStruct(s, d) for s, d in out_shapes),
            in_specs=[vmem_spec] * 17,
            out_specs=(any_spec,) * 16,
            scratch_shapes=[pltpu.VMEM(s, d) for s, d in out_shapes] + [dma((SEMS,))],
            compiler_params=pltpu.CompilerParams(vmem_limit_bytes=16 * 1024 * 1024),
            name="adamw_update",
        )(*(pltpu.with_memory_space_constraint(r, pltpu.VMEM) for r in results))

    in_specs = (grad_four, grad_three, grad_three, grad_three,
                layer_spec, layer_spec, layer_spec, down_spec, down_spec, down_spec,
                norm_spec, norm_spec, norm_spec, embed_spec, embed_spec, embed_spec)
    out_specs = (layer_spec,) * 4 + (down_spec,) * 4 + (norm_spec,) * 4 + (embed_spec,) * 4
    return jax.shard_map(local_update, mesh=mesh, in_specs=in_specs, out_specs=out_specs, check_vma=False)
```

```python
import jax
import jax.numpy as jnp
from jax import lax
from jax.experimental import pallas as pl
from jax.experimental.pallas import tpu as pltpu
from jax.sharding import PartitionSpec as P

ADAM_BETA1 = 0.9
ADAM_BETA2 = 0.95
ADAM_EPS = 1e-8
LEARN_RATE = 4e-4
WEIGHT_DECAY = 0.1
CLIP_EPS = 1e-6
OPT_STEP = 20
BIAS_ONE = 1.0 - ADAM_BETA1 ** OPT_STEP
BIAS_TWO = 1.0 - ADAM_BETA2 ** OPT_STEP

MESH = pl.DeviceIdType.MESH
LAYER, DOWN, NORM, EMBED = range(4)
DECAYS = (WEIGHT_DECAY, WEIGHT_DECAY, WEIGHT_DECAY, 0.0)
SHARES = ((6, 64, 896), (64, 4864), (4, 224), (64, 896))
WINDOWS = ((6, 64, 896), (64, 4864), (4, 384), (64, 896))
EARLY = 32
HALF = EARLY // 2
PIECES = range(0, HALF, 8)

GROUPS = ([(EMBED, None, slice(EARLY, EARLY + 8)), (EMBED, None, slice(0, EARLY)), (EMBED, None, slice(EARLY + 8, 64)),
           (LAYER, 0, None), (NORM, None, None)]
          + [(DOWN, None, slice(r, r + 8)) for r in range(0, 64, 8)] + [(LAYER, l, None) for l in range(1, 6)])
STAGED = 4
PAIR_AHEAD = 4
PAIR_RING = 2 * PAIR_AHEAD


def plan():
    chunks = [(EMBED, (slice(r, r + 8),), 0 if r == EARLY else 2) for r in range(EARLY, 64, 8)]
    chunks += [(LAYER, (0, slice(r, r + 8)), 3) for r in range(0, 64, 8)]
    chunks.append((NORM, (), 4))
    cuts = (0, 1024, 2048, 3072, 3968, 4864)
    chunks += [(DOWN, (slice(r, r + 8), slice(a, b)), 5 + r // 8) for r in range(0, 64, 8) for a, b in zip(cuts, cuts[1:])]
    chunks += [(LAYER, (l, slice(r, r + 8)), 12 + l) for l in range(1, 6) for r in range(0, 64, 8)]
    return chunks


CHUNKS = plan()
X_AHEAD, Y_BEHIND = 6, 5
X_RING, Y_RING = 2 * X_AHEAD + 2, 2 * Y_BEHIND + 2
EARLY_STEPS = {11: 0, 15: 1}


def at(ref, index):
    return ref.at[tuple(pl.ds(i.start, i.stop - i.start) if isinstance(i, slice) else i for i in index)] if index else ref


def tile_sum(value):
    rows, columns = value.shape
    parts = [value[r:r + 8, c:c + 128] for r in range(0, rows, 8) for c in range(0, columns, 128)]
    while len(parts) > 1:
        parts = [a + b for a, b in zip(parts[::2], parts[1::2])] + parts[len(parts) // 2 * 2:]
    return parts[0]


def reduce_kernel(*refs):
    grads, states = refs[:4], refs[4:16]
    means, copies, clip = refs[16:20], refs[20:32], refs[32]
    far, near, x_in, y_in = (refs[33 + 4 * i:37 + 4 * i] for i in range(4))
    (first, raw_in, early_in, norms, acc, first_sem, group_sem, state_sem, send_sem, x_recv, y_recv,
     early_recv, early_x, early_y, raw_recv, norm_recv) = refs[49:]

    dp, me = lax.axis_index("dp"), lax.axis_index("fsdp")
    partner = me + 1 - 2 * lax.rem(me, 2)
    across = lax.rem(me + 2, 4)
    diagonal = lax.rem(partner + 2, 4)
    other = 1 - dp
    peers = ((dp, across), (dp, diagonal), (dp, partner))
    held = (far, near)

    def share(array, fsdp, layer=None, rows=None):
        ref = grads[array].at[0]
        if array == NORM:
            start = jnp.minimum((fsdp * 7) // 4, 4)
            return ref.at[:, pl.ds(pl.multiple_of(start * 128, 128), 384)]
        rows = rows or slice(0, 64)
        window = pl.ds(pl.multiple_of(fsdp * 64 + rows.start, 8), rows.stop - rows.start)
        return ref.at[layer, window, :] if array == LAYER else ref.at[window, :]

    def slot(which, g, i):
        array, layer, rows = GROUPS[g]
        ref = held[which][array]
        lead = i if i is not None else slice(0, 2)
        return at(ref, (lead, layer) if array == LAYER else (lead, rows) if rows is not None else (lead,))

    def load(which, g):
        array, layer, rows = GROUPS[g]
        return pltpu.make_async_copy(
            share(array, (across, me)[which], layer, rows), slot(which, g, 0), group_sem.at[which, g % PAIR_RING])

    def stage(which, i):
        return pltpu.make_async_copy(
            share((EMBED, LAYER)[i], (diagonal, partner)[which], 0), first.at[i, which], first_sem.at[i])

    def pair(which, g):
        array, layer, rows = GROUPS[g]
        return pltpu.make_async_remote_copy(
            src_ref=share(array, (diagonal, partner)[which], layer, rows) if g >= STAGED else at(first, (int(array == LAYER), which) + (() if rows is None else (rows,))),
            dst_ref=slot(which, g, 1), send_sem=send_sem, recv_sem=group_sem.at[which, g % PAIR_RING],
            device_id=(dp, partner), device_id_type=MESH)

    def over_x(c):
        array, index, _ = CHUNKS[c]
        return pltpu.make_async_remote_copy(
            src_ref=at(far[array].at[0], index), dst_ref=at(x_in[array], index),
            send_sem=send_sem, recv_sem=x_recv.at[c % X_RING], device_id=(dp, across), device_id_type=MESH)

    def raw():
        return pltpu.make_async_remote_copy(
            src_ref=first.at[0, 0, pl.ds(EARLY, 8), :], dst_ref=raw_in, send_sem=send_sem, recv_sem=raw_recv,
            device_id=(dp, diagonal), device_id_type=MESH)

    def over_y(c):
        array, index, _ = CHUNKS[c]
        return pltpu.make_async_remote_copy(
            src_ref=at(near[array].at[0], index), dst_ref=at(y_in[array], index),
            send_sem=send_sem, recv_sem=y_recv.at[c % Y_RING], device_id=(other, me), device_id_type=MESH)

    def half(owner, piece=None):
        start, size = (0, HALF) if piece is None else (PIECES[piece], 8)
        return pl.ds(pl.multiple_of(owner * HALF + start, 8), size)

    def early(which):
        return pltpu.make_async_remote_copy(
            src_ref=held[which][EMBED].at[0, half(other), :], dst_ref=early_in.at[which],
            send_sem=send_sem, recv_sem=early_recv.at[which], device_id=(other, me), device_id_type=MESH)

    def early_over_x(piece):
        return pltpu.make_async_remote_copy(
            src_ref=far[EMBED].at[0, half(dp, piece), :], dst_ref=x_in[EMBED].at[half(dp, piece), :],
            send_sem=send_sem, recv_sem=early_x.at[piece], device_id=(dp, across), device_id_type=MESH)

    def early_over_y(piece, owner):
        return pltpu.make_async_remote_copy(
            src_ref=near[EMBED].at[0, half(owner, piece), :], dst_ref=y_in[EMBED].at[half(owner, piece), :],
            send_sem=send_sem, recv_sem=early_y.at[piece], device_id=(other, me), device_id_type=MESH)

    def norm_to(i):
        return pltpu.make_async_remote_copy(
            src_ref=norms.at[me, pl.ds(0, 1), :], dst_ref=norms.at[me, pl.ds(0, 1), :], send_sem=send_sem, recv_sem=norm_recv.at[i],
            device_id=peers[i], device_id_type=MESH)

    barrier = pltpu.get_barrier_semaphore()
    for device in ((other, me),) + peers:
        pl.semaphore_signal(barrier, inc=1, device_id=device, device_id_type=MESH)
    for i in (0, 1):
        for which in (0, 1):
            stage(which, i).start()
    for g in range(PAIR_AHEAD):
        for which in (0, 1):
            load(which, g).start()
    acc[...] = jnp.zeros_like(acc)
    pltpu.make_async_copy(first.at[0], first.at[0], first_sem.at[0]).wait()
    pl.semaphore_wait(barrier, 4)
    ready = set()

    def need(which, g):
        if (which, g) not in ready:
            ready.add((which, g))
            ref = slot(which, g, None if (which, g) != (0, 0) else 0)
            pltpu.make_async_copy(ref, ref, group_sem.at[which, g % PAIR_RING]).wait()
            if g + PAIR_AHEAD < len(GROUPS):
                pair(which, g + PAIR_AHEAD).start()
                load(which, g + PAIR_AHEAD).start()

    need(0, 0)
    over_x(0).start()
    raw().start()
    for which, g in ((0, 1), (0, 2), (1, 1), (1, 0), (1, 2)):
        pair(which, g).start()
    pltpu.make_async_copy(first.at[1], first.at[1], first_sem.at[1]).wait()
    for which in (0, 1):
        pair(which, 3).start()
    for s, d in zip(states, copies):
        pltpu.make_async_copy(s, d, state_sem).start()


    def send_x(c):
        if c == 0:
            return
        array, index, g = CHUNKS[c]
        need(0, g)
        ref = at(far[array].at[0], index)
        ref[...] = ref[...] + at(far[array].at[1], index)[...]
        over_x(c).start()

    def send_y(c):
        array, index, g = CHUNKS[c]
        need(1, g)
        over_x(c).wait_recv()
        ref = at(near[array].at[0], index)
        total = (ref[...] + at(near[array].at[1], index)[...]) + at(x_in[array], index)[...]
        if c == 0:
            raw().wait_recv()
            total = total + raw_in[...]
        ref[...] = total
        over_y(c).start()

    def finish(c):
        array, index, _ = CHUNKS[c]
        over_y(c).wait_recv()
        mean = (at(near[array].at[0], index)[...] + at(y_in[array], index)[...]) * (1.0 / 8.0)
        if array == NORM:
            for f, skip in enumerate((0, 96, 64, 160)):
                @pl.when(me == f)
                def _():
                    mine = pltpu.roll(mean, (384 - skip) % 384, axis=1)
                    mine = jnp.where(lax.broadcasted_iota(jnp.int32, (4, 384), 1) < 224, mine, 0.0)
                    means[NORM][...] = mine[:, :224]
                    square = mine * mine
                    acc[0:4, :] = acc[0:4, :] + (square[:, :128] + square[:, 128:256])
        else:
            at(means[array], index)[...] = mean
            total = acc[...] + tile_sum(mean * mean)
            if c < len(CHUNKS) - 1:
                acc[...] = total
            else:
                norms[me, 0:1, :] = jnp.sum(total, axis=0, keepdims=True)

    def send_early(which):
        need(which, 1)
        ref = held[which][EMBED]
        for owner in (other, dp):
            ref[0, half(owner), :] = ref[0, half(owner), :] + ref[1, half(owner), :]
            if owner is other:
                early(which).start()

    def send_early_x(piece):
        if piece == 0:
            early(0).wait_recv()
        rows = half(dp, piece)
        far[EMBED][0, rows, :] = far[EMBED][0, rows, :] + early_in[0, PIECES[piece]:PIECES[piece] + 8, :]
        early_over_x(piece).start()

    def send_early_y(piece):
        if piece == 0:
            early(1).wait_recv()
        early_over_x(piece).wait_recv()
        rows = half(dp, piece)
        total = (near[EMBED][0, rows, :] + early_in[1, PIECES[piece]:PIECES[piece] + 8, :]) + x_in[EMBED][rows, :]
        near[EMBED][0, rows, :] = total
        means[EMBED][rows, :] = total * (1.0 / 8.0)
        early_over_y(piece, dp).start()

    def finish_early(piece):
        early_over_y(piece, other).wait_recv()
        rows = half(other, piece)
        means[EMBED][rows, :] = y_in[EMBED][rows, :] * (1.0 / 8.0)
        total = acc[...]
        for owner in (0, 1):
            mean = means[EMBED][half(owner, piece), :]
            total = total + tile_sum(mean * mean)
        acc[...] = total

    count = len(CHUNKS)
    for step in range(count + X_AHEAD + Y_BEHIND):
        if step < count:
            send_x(step)
        if step == 0:
            send_early(0)
            send_early(1)

            @pl.when(lax.rem(me, 2) == 1)
            def _():
                pl.delay(1800)
        if step in EARLY_STEPS:
            send_early_x(EARLY_STEPS[step])
        if 0 <= step - X_AHEAD < count:
            send_y(step - X_AHEAD)
        if step - X_AHEAD in EARLY_STEPS:
            send_early_y(EARLY_STEPS[step - X_AHEAD])
        if 0 <= step - X_AHEAD - Y_BEHIND < count:
            finish(step - X_AHEAD - Y_BEHIND)
        if step - X_AHEAD - Y_BEHIND in EARLY_STEPS:
            finish_early(EARLY_STEPS[step - X_AHEAD - Y_BEHIND])
    for i in range(3):
        norm_to(i).start()

    for s, d in zip(states, copies):
        pltpu.make_async_copy(s, d, state_sem).wait()
    for array in range(4):
        for which in (0, 1):
            ref = held[which][array].at[0]
            pltpu.make_async_remote_copy(
                src_ref=ref, dst_ref=ref, send_sem=send_sem, recv_sem=norm_recv.at[0],
                device_id=(dp, partner), device_id_type=MESH).wait_send()
        rows = slice(HALF, 64) if array == EMBED else None
        index = () if rows is None else (rows,)
        pltpu.make_async_remote_copy(
            src_ref=at(far[array].at[0], index), dst_ref=at(x_in[array], index), send_sem=send_sem, recv_sem=norm_recv.at[0],
            device_id=(dp, across), device_id_type=MESH).wait_send()
        pltpu.make_async_remote_copy(
            src_ref=near[array].at[0], dst_ref=y_in[array], send_sem=send_sem, recv_sem=norm_recv.at[0],
            device_id=(other, me), device_id_type=MESH).wait_send()
    early(0).wait_send()
    for i in range(3):
        norm_to(i).wait_send()
    for i in range(3):
        norm_to(i).wait_recv()
    rows = [norms[f, 0:1, :] for f in range(4)]
    total = jnp.sum((rows[0] + rows[1]) + (rows[2] + rows[3]), axis=1, keepdims=True)
    norm = jnp.sqrt(jnp.broadcast_to(total, (8, 128)))
    clip[...] = jnp.minimum(1.0, 1.0 / (norm + CLIP_EPS))


def adamw(mean, master, exp_avg, exp_avg_sq, clip, decay):
    clipped = clip * mean
    avg_new = ADAM_BETA1 * exp_avg + (1.0 - ADAM_BETA1) * clipped
    sq_new = ADAM_BETA2 * exp_avg_sq + (1.0 - ADAM_BETA2) * clipped * clipped
    step_dir = (avg_new / BIAS_ONE) / (jnp.sqrt(sq_new / BIAS_TWO) + ADAM_EPS)
    master_new = master - LEARN_RATE * (step_dir + decay * master)
    return master_new, avg_new, sq_new, master_new.astype(jnp.bfloat16)


def update_kernel(*refs):
    means, states, clip_ref = refs[:4], refs[4:16], refs[16]
    outs, bufs, sem = refs[17:33], refs[33:49], refs[49]
    clip = clip_ref[...]

    def rows(array, index):
        ins = [means[array]] + list(states[3 * array:3 * array + 3])
        ins = [r[index] for r in ins]
        height, width = ins[0].shape
        scale = jnp.concatenate([clip[:height]] * -(-width // 128), axis=1)[:, :width]
        for o, value in zip(bufs[4 * array:4 * array + 4], adamw(*ins, scale, DECAYS[array])):
            o[index] = value

    def send(array, index):
        for k in range(4 * array, 4 * array + 4):
            pltpu.make_async_copy(at(bufs[k], index), at(outs[k], index), sem.at[k % SEMS]).start()

    for r in range(0, 64, 8):
        rows(LAYER, (0, slice(r, r + 8)))
        send(LAYER, (0, slice(r, r + 8)))
    for l in range(1, 6):
        for r in range(0, 64, 8):
            rows(LAYER, (l, slice(r, r + 8)))
            if r % 32 == 24:
                send(LAYER, (l, slice(r - 24, r + 8)))
    for r in range(0, 64, 8):
        rows(DOWN, (slice(r, r + 8),))
        send(DOWN, (slice(r, r + 8),))
    for r in range(0, 64, 8):
        rows(EMBED, (slice(r, r + 8),))
    send(EMBED, ())
    rows(NORM, (slice(0, 4),))
    send(NORM, ())
    for k in range(16):
        pltpu.make_async_copy(bufs[k], outs[k], sem.at[k % SEMS]).wait()


SEMS = 1


def solution(mesh):
    grad_four = P(("dp", "fsdp"), None, None, None)
    grad_three = P(("dp", "fsdp"), None, None)
    layer_spec = P(None, "fsdp", None)
    down_spec = P("fsdp", None)
    norm_spec = P(None, "fsdp")
    embed_spec = P("fsdp", None)
    any_spec = pl.BlockSpec(memory_space=pl.ANY)
    vmem_spec = pl.BlockSpec(memory_space=pltpu.VMEM)
    dma = pltpu.SemaphoreType.DMA
    f32 = jnp.float32

    def local_update(*args):
        state_shapes = [s for s in SHARES for _ in range(3)]
        results = pl.pallas_call(
            reduce_kernel,
            out_shape=tuple(pltpu.VMEM(s, f32) for s in list(SHARES) + state_shapes + [(8, 128)]),
            in_specs=[any_spec] * 16,
            out_specs=(vmem_spec,) * 17,
            scratch_shapes=[pltpu.VMEM(lead + s, f32) for lead in ((2,), (2,), (), ()) for s in WINDOWS] + [
                pltpu.VMEM((2, 2, 64, 896), f32), pltpu.VMEM((8, 896), f32), pltpu.VMEM((2, HALF, 896), f32), pltpu.VMEM((4, 8, 128), f32), pltpu.VMEM((8, 128), f32),
                dma((2,)), dma((2, PAIR_RING)), dma, dma, dma((X_RING,)), dma((Y_RING,)),
                dma((2,)), dma((len(PIECES),)), dma((len(PIECES),)), dma, dma((3,)),
            ],
            compiler_params=pltpu.CompilerParams(
                collective_id=0, has_side_effects=True, vmem_limit_bytes=24 * 1024 * 1024),
            name="reduce_grads",
        )(*(pltpu.with_memory_space_constraint(a, pltpu.HBM) for a in args))
        out_shapes = [(s, d) for s in SHARES for d in (f32, f32, f32, jnp.bfloat16)]
        return pl.pallas_call(
            update_kernel,
            out_shape=tuple(jax.ShapeDtypeStruct(s, d) for s, d in out_shapes),
            in_specs=[vmem_spec] * 17,
            out_specs=(any_spec,) * 16,
            scratch_shapes=[pltpu.VMEM(s, d) for s, d in out_shapes] + [dma((SEMS,))],
            compiler_params=pltpu.CompilerParams(vmem_limit_bytes=16 * 1024 * 1024),
            name="adamw_update",
        )(*(pltpu.with_memory_space_constraint(r, pltpu.VMEM) for r in results))

    in_specs = (grad_four, grad_three, grad_three, grad_three,
                layer_spec, layer_spec, layer_spec, down_spec, down_spec, down_spec,
                norm_spec, norm_spec, norm_spec, embed_spec, embed_spec, embed_spec)
    out_specs = (layer_spec,) * 4 + (down_spec,) * 4 + (norm_spec,) * 4 + (embed_spec,) * 4
    return jax.shard_map(local_update, mesh=mesh, in_specs=in_specs, out_specs=out_specs, check_vma=False)
```

```python
import jax
import jax.numpy as jnp
from jax import lax
from jax.experimental import pallas as pl
from jax.experimental.pallas import tpu as pltpu
from jax.sharding import PartitionSpec as P

ADAM_BETA1 = 0.9
ADAM_BETA2 = 0.95
ADAM_EPS = 1e-8
LEARN_RATE = 4e-4
WEIGHT_DECAY = 0.1
CLIP_EPS = 1e-6
OPT_STEP = 20
BIAS_ONE = 1.0 - ADAM_BETA1 ** OPT_STEP
BIAS_TWO = 1.0 - ADAM_BETA2 ** OPT_STEP

MESH = pl.DeviceIdType.MESH
LAYER, DOWN, NORM, EMBED = range(4)
DECAYS = (WEIGHT_DECAY, WEIGHT_DECAY, WEIGHT_DECAY, 0.0)
SHARES = ((6, 64, 896), (64, 4864), (4, 224), (64, 896))
WINDOWS = ((6, 64, 896), (64, 4864), (4, 384), (64, 896))
EARLY = 32
HALF = EARLY // 2
PIECES = range(0, HALF, 8)

GROUPS = ([(EMBED, None, slice(EARLY, EARLY + 8)), (EMBED, None, slice(0, EARLY)), (EMBED, None, slice(EARLY + 8, 64)),
           (LAYER, 0, None), (NORM, None, None)]
          + [(DOWN, None, slice(r, r + 8)) for r in range(0, 64, 8)] + [(LAYER, l, None) for l in range(1, 6)])
STAGED = 4
PAIR_AHEAD = 4
PAIR_RING = 2 * PAIR_AHEAD


def plan():
    chunks = [(EMBED, (slice(r, r + 8),), 0 if r == EARLY else 2) for r in range(EARLY, 64, 8)]
    chunks += [(LAYER, (0, slice(r, r + 8)), 3) for r in range(0, 64, 8)]
    chunks.append((NORM, (), 4))
    cuts = (0, 1024, 2048, 3072, 3968, 4864)
    chunks += [(DOWN, (slice(r, r + 8), slice(a, b)), 5 + r // 8) for r in range(0, 64, 8) for a, b in zip(cuts, cuts[1:])]
    chunks += [(LAYER, (l, slice(r, r + 8)), 12 + l) for l in range(1, 6) for r in range(0, 64, 8)]
    return chunks


CHUNKS = plan()
X_AHEAD, Y_BEHIND = 6, 5
X_RING, Y_RING = 2 * X_AHEAD + 2, 2 * Y_BEHIND + 2
EARLY_STEPS = {11: 0, 15: 1}


def at(ref, index):
    return ref.at[tuple(pl.ds(i.start, i.stop - i.start) if isinstance(i, slice) else i for i in index)] if index else ref


def tile_sum(value):
    rows, columns = value.shape
    parts = [value[r:r + 8, c:c + 128] for r in range(0, rows, 8) for c in range(0, columns, 128)]
    while len(parts) > 1:
        parts = [a + b for a, b in zip(parts[::2], parts[1::2])] + parts[len(parts) // 2 * 2:]
    return parts[0]


def reduce_kernel(*refs):
    grads, states = refs[:4], refs[4:16]
    means, copies, clip = refs[16:20], refs[20:32], refs[32]
    far, near, x_in, y_in = (refs[33 + 4 * i:37 + 4 * i] for i in range(4))
    (first, raw_in, early_in, norms, acc, first_sem, group_sem, state_sem, send_sem, x_recv, y_recv,
     early_recv, norm_recv) = refs[49:]

    dp, me = lax.axis_index("dp"), lax.axis_index("fsdp")
    partner = me + 1 - 2 * lax.rem(me, 2)
    across = lax.rem(me + 2, 4)
    diagonal = lax.rem(partner + 2, 4)
    other = 1 - dp
    peers = ((dp, across), (dp, diagonal), (dp, partner))
    held = (far, near)

    def share(array, fsdp, layer=None, rows=None):
        ref = grads[array].at[0]
        if array == NORM:
            start = jnp.minimum((fsdp * 7) // 4, 4)
            return ref.at[:, pl.ds(pl.multiple_of(start * 128, 128), 384)]
        rows = rows or slice(0, 64)
        window = pl.ds(pl.multiple_of(fsdp * 64 + rows.start, 8), rows.stop - rows.start)
        return ref.at[layer, window, :] if array == LAYER else ref.at[window, :]

    def slot(which, g, i):
        array, layer, rows = GROUPS[g]
        ref = held[which][array]
        lead = i if i is not None else slice(0, 2)
        return at(ref, (lead, layer) if array == LAYER else (lead, rows) if rows is not None else (lead,))

    def load(which, g):
        array, layer, rows = GROUPS[g]
        return pltpu.make_async_copy(
            share(array, (across, me)[which], layer, rows), slot(which, g, 0), group_sem.at[which, g % PAIR_RING])

    def stage(which, i):
        return pltpu.make_async_copy(
            share((EMBED, LAYER)[i], (diagonal, partner)[which], 0), first.at[i, which], first_sem.at[i])

    def pair(which, g):
        array, layer, rows = GROUPS[g]
        return pltpu.make_async_remote_copy(
            src_ref=share(array, (diagonal, partner)[which], layer, rows) if g >= STAGED else at(first, (int(array == LAYER), which) + (() if rows is None else (rows,))),
            dst_ref=slot(which, g, 1), send_sem=send_sem, recv_sem=group_sem.at[which, g % PAIR_RING],
            device_id=(dp, partner), device_id_type=MESH)

    def over_x(c):
        array, index, _ = CHUNKS[c]
        return pltpu.make_async_remote_copy(
            src_ref=at(far[array].at[0], index), dst_ref=at(x_in[array], index),
            send_sem=send_sem, recv_sem=x_recv.at[c % X_RING], device_id=(dp, across), device_id_type=MESH)

    def raw():
        return pltpu.make_async_remote_copy(
            src_ref=first.at[0, 0, pl.ds(EARLY, 8), :], dst_ref=raw_in, send_sem=send_sem, recv_sem=norm_recv.at[2],
            device_id=(dp, diagonal), device_id_type=MESH)

    def over_y(c):
        array, index, _ = CHUNKS[c]
        return pltpu.make_async_remote_copy(
            src_ref=at(near[array].at[0], index), dst_ref=at(y_in[array], index),
            send_sem=send_sem, recv_sem=y_recv.at[c % Y_RING], device_id=(other, me), device_id_type=MESH)

    def half(owner, piece=None):
        start, size = (0, HALF) if piece is None else (PIECES[piece], 8)
        return pl.ds(pl.multiple_of(owner * HALF + start, 8), size)

    def early(which):
        return pltpu.make_async_remote_copy(
            src_ref=held[which][EMBED].at[0, half(other), :], dst_ref=early_in.at[which],
            send_sem=send_sem, recv_sem=early_recv.at[which], device_id=(other, me), device_id_type=MESH)

    def early_over_x(piece):
        return pltpu.make_async_remote_copy(
            src_ref=far[EMBED].at[0, half(dp, piece), :], dst_ref=x_in[EMBED].at[half(dp, piece), :],
            send_sem=send_sem, recv_sem=norm_recv.at[piece], device_id=(dp, across), device_id_type=MESH)

    def early_over_y(piece, owner):
        return pltpu.make_async_remote_copy(
            src_ref=near[EMBED].at[0, half(owner, piece), :], dst_ref=y_in[EMBED].at[half(owner, piece), :],
            send_sem=send_sem, recv_sem=early_recv.at[piece], device_id=(other, me), device_id_type=MESH)

    def norm_to(i):
        return pltpu.make_async_remote_copy(
            src_ref=norms.at[me, pl.ds(0, 1), :], dst_ref=norms.at[me, pl.ds(0, 1), :], send_sem=send_sem, recv_sem=norm_recv.at[i],
            device_id=peers[i], device_id_type=MESH)

    barrier = pltpu.get_barrier_semaphore()
    for device in ((other, me),) + peers:
        pl.semaphore_signal(barrier, inc=1, device_id=device, device_id_type=MESH)
    for i in (0, 1):
        for which in (0, 1):
            stage(which, i).start()
    for g in range(PAIR_AHEAD):
        for which in (0, 1):
            load(which, g).start()
    acc[...] = jnp.zeros_like(acc)
    pltpu.make_async_copy(first.at[0], first.at[0], first_sem.at[0]).wait()
    pl.semaphore_wait(barrier, 4)
    ready = set()

    def need(which, g):
        if (which, g) not in ready:
            ready.add((which, g))
            ref = slot(which, g, None if (which, g) != (0, 0) else 0)
            pltpu.make_async_copy(ref, ref, group_sem.at[which, g % PAIR_RING]).wait()
            if g + PAIR_AHEAD < len(GROUPS):
                pair(which, g + PAIR_AHEAD).start()
                load(which, g + PAIR_AHEAD).start()

    need(0, 0)
    over_x(0).start()
    raw().start()
    for which, g in ((0, 1), (0, 2), (1, 1), (1, 0), (1, 2)):
        pair(which, g).start()
    pltpu.make_async_copy(first.at[1], first.at[1], first_sem.at[1]).wait()
    for which in (0, 1):
        pair(which, 3).start()
    for s, d in zip(states, copies):
        pltpu.make_async_copy(s, d, state_sem).start()


    def send_x(c):
        if c == 0:
            return
        array, index, g = CHUNKS[c]
        need(0, g)
        ref = at(far[array].at[0], index)
        ref[...] = ref[...] + at(far[array].at[1], index)[...]
        over_x(c).start()

    def send_y(c):
        array, index, g = CHUNKS[c]
        need(1, g)
        over_x(c).wait_recv()
        ref = at(near[array].at[0], index)
        total = (ref[...] + at(near[array].at[1], index)[...]) + at(x_in[array], index)[...]
        if c == 0:
            raw().wait_recv()
            total = total + raw_in[...]
        ref[...] = total
        over_y(c).start()

    def finish(c):
        array, index, _ = CHUNKS[c]
        over_y(c).wait_recv()
        mean = (at(near[array].at[0], index)[...] + at(y_in[array], index)[...]) * (1.0 / 8.0)
        if array == NORM:
            for f, skip in enumerate((0, 96, 64, 160)):
                @pl.when(me == f)
                def _():
                    mine = pltpu.roll(mean, (384 - skip) % 384, axis=1)
                    mine = jnp.where(lax.broadcasted_iota(jnp.int32, (4, 384), 1) < 224, mine, 0.0)
                    means[NORM][...] = mine[:, :224]
                    square = mine * mine
                    acc[0:4, :] = acc[0:4, :] + (square[:, :128] + square[:, 128:256])
        else:
            at(means[array], index)[...] = mean
            total = acc[...] + tile_sum(mean * mean)
            if c < len(CHUNKS) - 1:
                acc[...] = total
            else:
                norms[me, 0:1, :] = jnp.sum(total, axis=0, keepdims=True)

    def send_early(which):
        need(which, 1)
        ref = held[which][EMBED]
        for owner in (other, dp):
            ref[0, half(owner), :] = ref[0, half(owner), :] + ref[1, half(owner), :]
            if owner is other:
                early(which).start()

    def send_early_x(piece):
        if piece == 0:
            early(0).wait_recv()
            early(1).wait_recv()
        rows = half(dp, piece)
        far[EMBED][0, rows, :] = far[EMBED][0, rows, :] + early_in[0, PIECES[piece]:PIECES[piece] + 8, :]
        early_over_x(piece).start()

    def send_early_y(piece):
        early_over_x(piece).wait_recv()
        rows = half(dp, piece)
        total = (near[EMBED][0, rows, :] + early_in[1, PIECES[piece]:PIECES[piece] + 8, :]) + x_in[EMBED][rows, :]
        near[EMBED][0, rows, :] = total
        means[EMBED][rows, :] = total * (1.0 / 8.0)
        early_over_y(piece, dp).start()

    def finish_early(piece):
        early_over_y(piece, other).wait_recv()
        rows = half(other, piece)
        means[EMBED][rows, :] = y_in[EMBED][rows, :] * (1.0 / 8.0)
        total = acc[...]
        for owner in (0, 1):
            mean = means[EMBED][half(owner, piece), :]
            total = total + tile_sum(mean * mean)
        acc[...] = total

    count = len(CHUNKS)
    for step in range(count + X_AHEAD + Y_BEHIND):
        if step < count:
            send_x(step)
        if step == 0:
            send_early(0)
            send_early(1)

            @pl.when(lax.rem(me, 2) == 1)
            def _():
                pl.delay(1800)
        if step in EARLY_STEPS:
            send_early_x(EARLY_STEPS[step])
        if 0 <= step - X_AHEAD < count:
            send_y(step - X_AHEAD)
        if step - X_AHEAD in EARLY_STEPS:
            send_early_y(EARLY_STEPS[step - X_AHEAD])
        if 0 <= step - X_AHEAD - Y_BEHIND < count:
            finish(step - X_AHEAD - Y_BEHIND)
        if step - X_AHEAD - Y_BEHIND in EARLY_STEPS:
            finish_early(EARLY_STEPS[step - X_AHEAD - Y_BEHIND])
    for i in range(3):
        norm_to(i).start()

    for s, d in zip(states, copies):
        pltpu.make_async_copy(s, d, state_sem).wait()
    for array in range(4):
        for which in (0, 1):
            ref = held[which][array].at[0]
            pltpu.make_async_remote_copy(
                src_ref=ref, dst_ref=ref, send_sem=send_sem, recv_sem=norm_recv.at[0],
                device_id=(dp, partner), device_id_type=MESH).wait_send()
        rows = slice(HALF, 64) if array == EMBED else None
        index = () if rows is None else (rows,)
        pltpu.make_async_remote_copy(
            src_ref=at(far[array].at[0], index), dst_ref=at(x_in[array], index), send_sem=send_sem, recv_sem=norm_recv.at[0],
            device_id=(dp, across), device_id_type=MESH).wait_send()
        pltpu.make_async_remote_copy(
            src_ref=near[array].at[0], dst_ref=y_in[array], send_sem=send_sem, recv_sem=norm_recv.at[0],
            device_id=(other, me), device_id_type=MESH).wait_send()
    early(0).wait_send()
    for i in range(3):
        norm_to(i).wait_send()
    for i in range(3):
        norm_to(i).wait_recv()
    rows = [norms[f, 0:1, :] for f in range(4)]
    total = jnp.sum((rows[0] + rows[1]) + (rows[2] + rows[3]), axis=1, keepdims=True)
    norm = jnp.sqrt(jnp.broadcast_to(total, (8, 128)))
    clip[...] = jnp.minimum(1.0, 1.0 / (norm + CLIP_EPS))


def adamw(mean, master, exp_avg, exp_avg_sq, clip, decay):
    clipped = clip * mean
    avg_new = ADAM_BETA1 * exp_avg + (1.0 - ADAM_BETA1) * clipped
    sq_new = ADAM_BETA2 * exp_avg_sq + (1.0 - ADAM_BETA2) * clipped * clipped
    step_dir = (avg_new / BIAS_ONE) / (jnp.sqrt(sq_new / BIAS_TWO) + ADAM_EPS)
    master_new = master - LEARN_RATE * (step_dir + decay * master)
    return master_new, avg_new, sq_new, master_new.astype(jnp.bfloat16)


def update_kernel(*refs):
    means, states, clip_ref = refs[:4], refs[4:16], refs[16]
    outs, bufs, sem = refs[17:33], refs[33:49], refs[49]
    clip = clip_ref[...]

    def rows(array, index):
        ins = [means[array]] + list(states[3 * array:3 * array + 3])
        ins = [r[index] for r in ins]
        height, width = ins[0].shape
        scale = jnp.concatenate([clip[:height]] * -(-width // 128), axis=1)[:, :width]
        for o, value in zip(bufs[4 * array:4 * array + 4], adamw(*ins, scale, DECAYS[array])):
            o[index] = value

    def send(array, index):
        for k in range(4 * array, 4 * array + 4):
            pltpu.make_async_copy(at(bufs[k], index), at(outs[k], index), sem.at[k % SEMS]).start()

    for r in range(0, 64, 8):
        rows(LAYER, (0, slice(r, r + 8)))
        send(LAYER, (0, slice(r, r + 8)))
    for l in range(1, 6):
        for r in range(0, 64, 8):
            rows(LAYER, (l, slice(r, r + 8)))
            if r % 32 == 24:
                send(LAYER, (l, slice(r - 24, r + 8)))
    for r in range(0, 64, 8):
        rows(DOWN, (slice(r, r + 8),))
        send(DOWN, (slice(r, r + 8),))
    for r in range(0, 64, 8):
        rows(EMBED, (slice(r, r + 8),))
    send(EMBED, ())
    rows(NORM, (slice(0, 4),))
    send(NORM, ())
    for k in range(16):
        pltpu.make_async_copy(bufs[k], outs[k], sem.at[k % SEMS]).wait()


SEMS = 1


def solution(mesh):
    grad_four = P(("dp", "fsdp"), None, None, None)
    grad_three = P(("dp", "fsdp"), None, None)
    layer_spec = P(None, "fsdp", None)
    down_spec = P("fsdp", None)
    norm_spec = P(None, "fsdp")
    embed_spec = P("fsdp", None)
    any_spec = pl.BlockSpec(memory_space=pl.ANY)
    vmem_spec = pl.BlockSpec(memory_space=pltpu.VMEM)
    dma = pltpu.SemaphoreType.DMA
    f32 = jnp.float32

    def local_update(*args):
        state_shapes = [s for s in SHARES for _ in range(3)]
        results = pl.pallas_call(
            reduce_kernel,
            out_shape=tuple(pltpu.VMEM(s, f32) for s in list(SHARES) + state_shapes + [(8, 128)]),
            in_specs=[any_spec] * 16,
            out_specs=(vmem_spec,) * 17,
            scratch_shapes=[pltpu.VMEM(lead + s, f32) for lead in ((2,), (2,), (), ()) for s in WINDOWS] + [
                pltpu.VMEM((2, 2, 64, 896), f32), pltpu.VMEM((8, 896), f32), pltpu.VMEM((2, HALF, 896), f32), pltpu.VMEM((4, 8, 128), f32), pltpu.VMEM((8, 128), f32),
                dma((2,)), dma((2, PAIR_RING)), dma, dma, dma((X_RING,)), dma((Y_RING,)),
                dma((2,)), dma((3,)),
            ],
            compiler_params=pltpu.CompilerParams(
                collective_id=0, has_side_effects=True, vmem_limit_bytes=24 * 1024 * 1024),
            name="reduce_grads",
        )(*(pltpu.with_memory_space_constraint(a, pltpu.HBM) for a in args))
        out_shapes = [(s, d) for s in SHARES for d in (f32, f32, f32, jnp.bfloat16)]
        return pl.pallas_call(
            update_kernel,
            out_shape=tuple(jax.ShapeDtypeStruct(s, d) for s, d in out_shapes),
            in_specs=[vmem_spec] * 17,
            out_specs=(any_spec,) * 16,
            scratch_shapes=[pltpu.VMEM(s, d) for s, d in out_shapes] + [dma((SEMS,))],
            compiler_params=pltpu.CompilerParams(vmem_limit_bytes=16 * 1024 * 1024),
            name="adamw_update",
        )(*(pltpu.with_memory_space_constraint(r, pltpu.VMEM) for r in results))

    in_specs = (grad_four, grad_three, grad_three, grad_three,
                layer_spec, layer_spec, layer_spec, down_spec, down_spec, down_spec,
                norm_spec, norm_spec, norm_spec, embed_spec, embed_spec, embed_spec)
    out_specs = (layer_spec,) * 4 + (down_spec,) * 4 + (norm_spec,) * 4 + (embed_spec,) * 4
    return jax.shard_map(local_update, mesh=mesh, in_specs=in_specs, out_specs=out_specs, check_vma=False)
```

```python
import jax
import jax.numpy as jnp
from jax import lax
from jax.experimental import pallas as pl
from jax.experimental.pallas import tpu as pltpu
from jax.sharding import PartitionSpec as P

ADAM_BETA1 = 0.9
ADAM_BETA2 = 0.95
ADAM_EPS = 1e-8
LEARN_RATE = 4e-4
WEIGHT_DECAY = 0.1
CLIP_EPS = 1e-6
OPT_STEP = 20
BIAS_ONE = 1.0 - ADAM_BETA1 ** OPT_STEP
BIAS_TWO = 1.0 - ADAM_BETA2 ** OPT_STEP

MESH = pl.DeviceIdType.MESH
LAYER, DOWN, NORM, EMBED = range(4)
DECAYS = (WEIGHT_DECAY, WEIGHT_DECAY, WEIGHT_DECAY, 0.0)
SHARES = ((6, 64, 896), (64, 4864), (4, 224), (64, 896))
WINDOWS = ((6, 64, 896), (64, 4864), (4, 384), (64, 896))
EARLY = 32
HALF = EARLY // 2
PIECES = range(0, HALF, 8)

GROUPS = ([(EMBED, None, slice(EARLY, EARLY + 8)), (EMBED, None, slice(0, EARLY)), (EMBED, None, slice(EARLY + 8, 64)),
           (LAYER, 0, None), (NORM, None, None)]
          + [(DOWN, None, slice(r, r + 8)) for r in range(0, 64, 8)] + [(LAYER, l, None) for l in range(1, 6)])
STAGED = 4
PAIR_AHEAD = 4
PAIR_RING = 2 * PAIR_AHEAD


def plan():
    chunks = [(EMBED, (slice(r, r + 8),), 0 if r == EARLY else 2) for r in range(EARLY, 64, 8)]
    chunks += [(LAYER, (0, slice(r, r + 8)), 3) for r in range(0, 64, 8)]
    chunks.append((NORM, (), 4))
    cuts = (0, 1024, 2048, 3072, 3968, 4864)
    chunks += [(DOWN, (slice(r, r + 8), slice(a, b)), 5 + r // 8) for r in range(0, 64, 8) for a, b in zip(cuts, cuts[1:])]
    chunks += [(LAYER, (l, slice(r, r + 8)), 12 + l) for l in range(1, 6) for r in range(0, 64, 8)]
    return chunks


CHUNKS = plan()
X_AHEAD, Y_BEHIND = 6, 5
X_RING, Y_RING = 2 * X_AHEAD + 2, 2 * Y_BEHIND + 2
EARLY_STEPS = {11: 0, 15: 1}


def at(ref, index):
    return ref.at[tuple(pl.ds(i.start, i.stop - i.start) if isinstance(i, slice) else i for i in index)] if index else ref


def tile_sum(value):
    rows, columns = value.shape
    parts = [value[r:r + 8, c:c + 128] for r in range(0, rows, 8) for c in range(0, columns, 128)]
    while len(parts) > 1:
        parts = [a + b for a, b in zip(parts[::2], parts[1::2])] + parts[len(parts) // 2 * 2:]
    return parts[0]


def reduce_kernel(*refs):
    grads, states = refs[:4], refs[4:16]
    means, copies, clip = refs[16:20], refs[20:32], refs[32]
    far, near, x_in, y_in = (refs[33 + 4 * i:37 + 4 * i] for i in range(4))
    (first, raw_in, early_in, norms, acc, first_sem, group_sem, send_sem, x_recv, y_recv,
     early_recv, norm_recv) = refs[49:]

    dp, me = lax.axis_index("dp"), lax.axis_index("fsdp")
    partner = me + 1 - 2 * lax.rem(me, 2)
    across = lax.rem(me + 2, 4)
    diagonal = lax.rem(partner + 2, 4)
    other = 1 - dp
    peers = ((dp, across), (dp, diagonal), (dp, partner))
    held = (far, near)

    def share(array, fsdp, layer=None, rows=None):
        ref = grads[array].at[0]
        if array == NORM:
            start = jnp.minimum((fsdp * 7) // 4, 4)
            return ref.at[:, pl.ds(pl.multiple_of(start * 128, 128), 384)]
        rows = rows or slice(0, 64)
        window = pl.ds(pl.multiple_of(fsdp * 64 + rows.start, 8), rows.stop - rows.start)
        return ref.at[layer, window, :] if array == LAYER else ref.at[window, :]

    def slot(which, g, i):
        array, layer, rows = GROUPS[g]
        ref = held[which][array]
        lead = i if i is not None else slice(0, 2)
        return at(ref, (lead, layer) if array == LAYER else (lead, rows) if rows is not None else (lead,))

    def load(which, g):
        array, layer, rows = GROUPS[g]
        return pltpu.make_async_copy(
            share(array, (across, me)[which], layer, rows), slot(which, g, 0), group_sem.at[which, g % PAIR_RING])

    def stage(which, i):
        return pltpu.make_async_copy(
            share((EMBED, LAYER)[i], (diagonal, partner)[which], 0), first.at[i, which], first_sem.at[i])

    def pair(which, g):
        array, layer, rows = GROUPS[g]
        return pltpu.make_async_remote_copy(
            src_ref=share(array, (diagonal, partner)[which], layer, rows) if g >= STAGED else at(first, (int(array == LAYER), which) + (() if rows is None else (rows,))),
            dst_ref=slot(which, g, 1), send_sem=send_sem, recv_sem=group_sem.at[which, g % PAIR_RING],
            device_id=(dp, partner), device_id_type=MESH)

    def over_x(c):
        array, index, _ = CHUNKS[c]
        return pltpu.make_async_remote_copy(
            src_ref=at(far[array].at[0], index), dst_ref=at(x_in[array], index),
            send_sem=send_sem, recv_sem=x_recv.at[c % X_RING], device_id=(dp, across), device_id_type=MESH)

    def raw():
        return pltpu.make_async_remote_copy(
            src_ref=first.at[0, 0, pl.ds(EARLY, 8), :], dst_ref=raw_in, send_sem=send_sem, recv_sem=norm_recv.at[2],
            device_id=(dp, diagonal), device_id_type=MESH)

    def over_y(c):
        array, index, _ = CHUNKS[c]
        return pltpu.make_async_remote_copy(
            src_ref=at(near[array].at[0], index), dst_ref=at(y_in[array], index),
            send_sem=send_sem, recv_sem=y_recv.at[c % Y_RING], device_id=(other, me), device_id_type=MESH)

    def half(owner, piece=None):
        start, size = (0, HALF) if piece is None else (PIECES[piece], 8)
        return pl.ds(pl.multiple_of(owner * HALF + start, 8), size)

    def early(which):
        return pltpu.make_async_remote_copy(
            src_ref=held[which][EMBED].at[0, half(other), :], dst_ref=early_in.at[which],
            send_sem=send_sem, recv_sem=early_recv.at[which], device_id=(other, me), device_id_type=MESH)

    def early_over_x(piece):
        return pltpu.make_async_remote_copy(
            src_ref=far[EMBED].at[0, half(dp, piece), :], dst_ref=x_in[EMBED].at[half(dp, piece), :],
            send_sem=send_sem, recv_sem=norm_recv.at[piece], device_id=(dp, across), device_id_type=MESH)

    def early_over_y(piece, owner):
        return pltpu.make_async_remote_copy(
            src_ref=near[EMBED].at[0, half(owner, piece), :], dst_ref=y_in[EMBED].at[half(owner, piece), :],
            send_sem=send_sem, recv_sem=early_recv.at[piece], device_id=(other, me), device_id_type=MESH)

    def norm_to(i):
        return pltpu.make_async_remote_copy(
            src_ref=norms.at[me, pl.ds(0, 1), :], dst_ref=norms.at[me, pl.ds(0, 1), :], send_sem=send_sem, recv_sem=norm_recv.at[i],
            device_id=peers[i], device_id_type=MESH)

    barrier = pltpu.get_barrier_semaphore()
    for device in ((other, me),) + peers:
        pl.semaphore_signal(barrier, inc=1, device_id=device, device_id_type=MESH)
    for i in (0, 1):
        for which in (0, 1):
            stage(which, i).start()
    for g in range(PAIR_AHEAD):
        for which in (0, 1):
            load(which, g).start()
    acc[...] = jnp.zeros_like(acc)
    pltpu.make_async_copy(first.at[0], first.at[0], first_sem.at[0]).wait()
    pl.semaphore_wait(barrier, 4)
    ready = set()

    def need(which, g):
        if (which, g) not in ready:
            ready.add((which, g))
            ref = slot(which, g, None if (which, g) != (0, 0) else 0)
            pltpu.make_async_copy(ref, ref, group_sem.at[which, g % PAIR_RING]).wait()
            if g + PAIR_AHEAD < len(GROUPS):
                pair(which, g + PAIR_AHEAD).start()
                load(which, g + PAIR_AHEAD).start()

    need(0, 0)
    over_x(0).start()
    raw().start()
    for which, g in ((0, 1), (0, 2), (1, 1), (1, 0), (1, 2)):
        pair(which, g).start()
    pltpu.make_async_copy(first.at[1], first.at[1], first_sem.at[1]).wait()
    for which in (0, 1):
        pair(which, 3).start()
    for s, d in zip(states, copies):
        pltpu.make_async_copy(s, d, send_sem).start()


    def send_x(c):
        if c == 0:
            return
        array, index, g = CHUNKS[c]
        need(0, g)
        ref = at(far[array].at[0], index)
        ref[...] = ref[...] + at(far[array].at[1], index)[...]
        over_x(c).start()

    def send_y(c):
        array, index, g = CHUNKS[c]
        need(1, g)
        over_x(c).wait_recv()
        ref = at(near[array].at[0], index)
        total = (ref[...] + at(near[array].at[1], index)[...]) + at(x_in[array], index)[...]
        if c == 0:
            raw().wait_recv()
            total = total + raw_in[...]
        ref[...] = total
        over_y(c).start()

    def finish(c):
        array, index, _ = CHUNKS[c]
        over_y(c).wait_recv()
        mean = (at(near[array].at[0], index)[...] + at(y_in[array], index)[...]) * (1.0 / 8.0)
        if array == NORM:
            for f, skip in enumerate((0, 96, 64, 160)):
                @pl.when(me == f)
                def _():
                    mine = pltpu.roll(mean, (384 - skip) % 384, axis=1)
                    mine = jnp.where(lax.broadcasted_iota(jnp.int32, (4, 384), 1) < 224, mine, 0.0)
                    means[NORM][...] = mine[:, :224]
                    square = mine * mine
                    acc[0:4, :] = acc[0:4, :] + (square[:, :128] + square[:, 128:256])
        else:
            at(means[array], index)[...] = mean
            total = acc[...] + tile_sum(mean * mean)
            if c < len(CHUNKS) - 1:
                acc[...] = total
            else:
                norms[me, 0:1, :] = jnp.sum(total, axis=0, keepdims=True)

    def send_early(which):
        need(which, 1)
        ref = held[which][EMBED]
        for owner in (other, dp):
            ref[0, half(owner), :] = ref[0, half(owner), :] + ref[1, half(owner), :]
            if owner is other:
                early(which).start()

    def send_early_x(piece):
        if piece == 0:
            early(0).wait_recv()
            early(1).wait_recv()
        rows = half(dp, piece)
        far[EMBED][0, rows, :] = far[EMBED][0, rows, :] + early_in[0, PIECES[piece]:PIECES[piece] + 8, :]
        early_over_x(piece).start()

    def send_early_y(piece):
        early_over_x(piece).wait_recv()
        rows = half(dp, piece)
        total = (near[EMBED][0, rows, :] + early_in[1, PIECES[piece]:PIECES[piece] + 8, :]) + x_in[EMBED][rows, :]
        near[EMBED][0, rows, :] = total
        means[EMBED][rows, :] = total * (1.0 / 8.0)
        early_over_y(piece, dp).start()

    def finish_early(piece):
        early_over_y(piece, other).wait_recv()
        rows = half(other, piece)
        means[EMBED][rows, :] = y_in[EMBED][rows, :] * (1.0 / 8.0)
        total = acc[...]
        for owner in (0, 1):
            mean = means[EMBED][half(owner, piece), :]
            total = total + tile_sum(mean * mean)
        acc[...] = total

    count = len(CHUNKS)
    for step in range(count + X_AHEAD + Y_BEHIND):
        if step < count:
            send_x(step)
        if step == 0:
            send_early(0)
            send_early(1)

            @pl.when(lax.rem(me, 2) == 1)
            def _():
                pl.delay(1800)
        if step in EARLY_STEPS:
            send_early_x(EARLY_STEPS[step])
        if 0 <= step - X_AHEAD < count:
            send_y(step - X_AHEAD)
        if step - X_AHEAD in EARLY_STEPS:
            send_early_y(EARLY_STEPS[step - X_AHEAD])
        if 0 <= step - X_AHEAD - Y_BEHIND < count:
            finish(step - X_AHEAD - Y_BEHIND)
        if step - X_AHEAD - Y_BEHIND in EARLY_STEPS:
            finish_early(EARLY_STEPS[step - X_AHEAD - Y_BEHIND])
    for i in range(3):
        norm_to(i).start()

    for s, d in zip(states, copies):
        pltpu.make_async_copy(s, d, send_sem).wait()
    for array in range(4):
        for which in (0, 1):
            ref = held[which][array].at[0]
            pltpu.make_async_remote_copy(
                src_ref=ref, dst_ref=ref, send_sem=send_sem, recv_sem=norm_recv.at[0],
                device_id=(dp, partner), device_id_type=MESH).wait_send()
        rows = slice(HALF, 64) if array == EMBED else None
        index = () if rows is None else (rows,)
        pltpu.make_async_remote_copy(
            src_ref=at(far[array].at[0], index), dst_ref=at(x_in[array], index), send_sem=send_sem, recv_sem=norm_recv.at[0],
            device_id=(dp, across), device_id_type=MESH).wait_send()
        pltpu.make_async_remote_copy(
            src_ref=near[array].at[0], dst_ref=y_in[array], send_sem=send_sem, recv_sem=norm_recv.at[0],
            device_id=(other, me), device_id_type=MESH).wait_send()
    early(0).wait_send()
    for i in range(3):
        norm_to(i).wait_send()
    for i in range(3):
        norm_to(i).wait_recv()
    rows = [norms[f, 0:1, :] for f in range(4)]
    total = jnp.sum((rows[0] + rows[1]) + (rows[2] + rows[3]), axis=1, keepdims=True)
    norm = jnp.sqrt(jnp.broadcast_to(total, (8, 128)))
    clip[...] = jnp.minimum(1.0, 1.0 / (norm + CLIP_EPS))


def adamw(mean, master, exp_avg, exp_avg_sq, clip, decay):
    clipped = clip * mean
    avg_new = ADAM_BETA1 * exp_avg + (1.0 - ADAM_BETA1) * clipped
    sq_new = ADAM_BETA2 * exp_avg_sq + (1.0 - ADAM_BETA2) * clipped * clipped
    step_dir = (avg_new / BIAS_ONE) / (jnp.sqrt(sq_new / BIAS_TWO) + ADAM_EPS)
    master_new = master - LEARN_RATE * (step_dir + decay * master)
    return master_new, avg_new, sq_new, master_new.astype(jnp.bfloat16)


def update_kernel(*refs):
    means, states, clip_ref = refs[:4], refs[4:16], refs[16]
    outs, bufs, sem = refs[17:33], refs[33:49], refs[49]
    clip = clip_ref[...]

    def rows(array, index):
        ins = [means[array]] + list(states[3 * array:3 * array + 3])
        ins = [r[index] for r in ins]
        height, width = ins[0].shape
        scale = jnp.concatenate([clip[:height]] * -(-width // 128), axis=1)[:, :width]
        for o, value in zip(bufs[4 * array:4 * array + 4], adamw(*ins, scale, DECAYS[array])):
            o[index] = value

    def send(array, index):
        for k in range(4 * array, 4 * array + 4):
            pltpu.make_async_copy(at(bufs[k], index), at(outs[k], index), sem.at[k % SEMS]).start()

    for r in range(0, 64, 8):
        rows(LAYER, (0, slice(r, r + 8)))
        send(LAYER, (0, slice(r, r + 8)))
    for l in range(1, 6):
        for r in range(0, 64, 8):
            rows(LAYER, (l, slice(r, r + 8)))
            if r % 32 == 24:
                send(LAYER, (l, slice(r - 24, r + 8)))
    for r in range(0, 64, 8):
        rows(DOWN, (slice(r, r + 8),))
        send(DOWN, (slice(r, r + 8),))
    for r in range(0, 64, 8):
        rows(EMBED, (slice(r, r + 8),))
    send(EMBED, ())
    rows(NORM, (slice(0, 4),))
    send(NORM, ())
    for k in range(16):
        pltpu.make_async_copy(bufs[k], outs[k], sem.at[k % SEMS]).wait()


SEMS = 1


def solution(mesh):
    grad_four = P(("dp", "fsdp"), None, None, None)
    grad_three = P(("dp", "fsdp"), None, None)
    layer_spec = P(None, "fsdp", None)
    down_spec = P("fsdp", None)
    norm_spec = P(None, "fsdp")
    embed_spec = P("fsdp", None)
    any_spec = pl.BlockSpec(memory_space=pl.ANY)
    vmem_spec = pl.BlockSpec(memory_space=pltpu.VMEM)
    dma = pltpu.SemaphoreType.DMA
    f32 = jnp.float32

    def local_update(*args):
        state_shapes = [s for s in SHARES for _ in range(3)]
        results = pl.pallas_call(
            reduce_kernel,
            out_shape=tuple(pltpu.VMEM(s, f32) for s in list(SHARES) + state_shapes + [(8, 128)]),
            in_specs=[any_spec] * 16,
            out_specs=(vmem_spec,) * 17,
            scratch_shapes=[pltpu.VMEM(lead + s, f32) for lead in ((2,), (2,), (), ()) for s in WINDOWS] + [
                pltpu.VMEM((2, 2, 64, 896), f32), pltpu.VMEM((8, 896), f32), pltpu.VMEM((2, HALF, 896), f32), pltpu.VMEM((4, 8, 128), f32), pltpu.VMEM((8, 128), f32),
                dma((2,)), dma((2, PAIR_RING)), dma, dma((X_RING,)), dma((Y_RING,)),
                dma((2,)), dma((3,)),
            ],
            compiler_params=pltpu.CompilerParams(
                collective_id=0, has_side_effects=True, vmem_limit_bytes=24 * 1024 * 1024),
            name="reduce_grads",
        )(*(pltpu.with_memory_space_constraint(a, pltpu.HBM) for a in args))
        out_shapes = [(s, d) for s in SHARES for d in (f32, f32, f32, jnp.bfloat16)]
        return pl.pallas_call(
            update_kernel,
            out_shape=tuple(jax.ShapeDtypeStruct(s, d) for s, d in out_shapes),
            in_specs=[vmem_spec] * 17,
            out_specs=(any_spec,) * 16,
            scratch_shapes=[pltpu.VMEM(s, d) for s, d in out_shapes] + [dma((SEMS,))],
            compiler_params=pltpu.CompilerParams(vmem_limit_bytes=16 * 1024 * 1024),
            name="adamw_update",
        )(*(pltpu.with_memory_space_constraint(r, pltpu.VMEM) for r in results))

    in_specs = (grad_four, grad_three, grad_three, grad_three,
                layer_spec, layer_spec, layer_spec, down_spec, down_spec, down_spec,
                norm_spec, norm_spec, norm_spec, embed_spec, embed_spec, embed_spec)
    out_specs = (layer_spec,) * 4 + (down_spec,) * 4 + (norm_spec,) * 4 + (embed_spec,) * 4
    return jax.shard_map(local_update, mesh=mesh, in_specs=in_specs, out_specs=out_specs, check_vma=False)
```
